128 devices in a mesh: gx: 8 (over y, core), gy: 16 (over x, z).
Axes of the slice: x: 4, y: 4, z: 4, core: 2. Of those that a mesh axis runs over, the one named last changes fastest.
Arguments:
- southward_speed_field: bfloat16 [75, 1024, 4096], P(None, 'gy', 'gx'), may hold values from -6 to 6
- thermal_anomaly: bfloat16 [75, 1024, 4096], P(None, 'gy', 'gx'), may hold values from -6 to 6
- section_surface: float32 [75, 1024, 4096], P(None, 'gy', 'gx'), may hold values from 0.3 to 3
- parallel_band_label: int32 [1024, 4096], P('gy', 'gx'), may hold values from 0 to 1799, as said below
- ocean_region_label: int32 [1024, 4096], P('gy', 'gx'), may hold values from 0 to 3
Outputs:
- heat_level: float32 [5, 75, 1800], replicated
- heat_total: float32 [5, 1800], replicated
The draws below stay inside these ranges and needn't reach their ends.
Inputs may be any that keep to these rules, and one draw needn't show every extreme that they name: `parallel_band_label`: let the owner of bin b be b // 113. All cells of an aligned run of 128 cells of one grid row (columns 128 m to 128 m + 127) have bins of one owner. Of the runs in one device's tile of 64 x 512 cells, at most 32 have bins of any one owner, and in every draw one owner has exactly 32 runs in every tile.
All inputs are finite; a program needn't handle non-finite values.
Results may differ from the reference program's by a relative error of at most 0.006.
Values may be sent and summed in bfloat16 or wider, within the bound.
No kernel may reach another device: no remote copies, remote signals or barrier semaphores. Data moves between devices by JAX's collectives and lax.ppermute only.
A program may use at most 128 MiB of HBM per device.

```python
import math
import jax
import jax.numpy as jnp

VERTICAL_LAYERS = 75
CY = 64
CX = 512
BINS = 1800
MERIDIONAL_SPANS = 1024
ZONAL_POSITIONS = 4096
BLK = 256
OWN = 113
CAP = 32
N_GX = 8
N_GY = 16


def draw_parallel_band_label(key, part):
    device_total = N_GX * N_GY
    slot_total = N_GY * CAP
    key_list = jax.random.split(key, 7)
    forced = jax.random.randint(key_list[0], (), 0, N_GY)
    weight = jax.random.randint(key_list[1], (device_total, N_GY), 0, 4) * 4096
    jitter = jax.random.randint(key_list[2], (device_total, slot_total), 0, 4096)
    slot_owner = (jnp.arange(slot_total) // CAP).astype(jnp.int32)
    priority = jnp.where(slot_owner == forced, 1 << 20, 0)
    scores = (jnp.take(weight, slot_owner, axis=1) + jitter + priority[None, :]) * slot_total + (slot_total - 1 - jnp.arange(slot_total))[None, :]
    ranking = jnp.argsort(-scores, axis=1)[:, :BLK]
    chosen = jnp.take(slot_owner, ranking)
    shuffle_keys = jax.random.randint(key_list[3], (device_total, BLK), 0, 1 << 20) * BLK + jnp.arange(BLK)[None, :]
    shuffle = jnp.argsort(shuffle_keys, axis=1)
    block_owner = jnp.take_along_axis(chosen, shuffle, axis=1)
    bin_count = jnp.minimum(OWN, BINS - block_owner * OWN)
    narrow = max(2, OWN // 8)
    wide_flag = jax.random.randint(key_list[4], (device_total, BLK), 0, 8) == 0
    spread = jnp.where(wide_flag, bin_count, jnp.minimum(bin_count, narrow))
    start_bin = jax.random.randint(key_list[5], (device_total, BLK), 0, 1 << 20) % (bin_count - spread + 1)
    offset = jax.random.randint(key_list[6], (device_total, BLK, 128), 0, 1 << 20) % spread[:, :, None]
    cell_bins = (block_owner * OWN + start_bin)[:, :, None] + offset
    cell_bins = cell_bins.reshape(N_GX, N_GY, CY, CX // 128, 128)
    cell_bins = jnp.transpose(cell_bins, (1, 2, 0, 3, 4)).reshape(MERIDIONAL_SPANS, ZONAL_POSITIONS)
    return cell_bins.astype(jnp.int32)


def plant(entries, own_key, smallest, top_value):
    longest = entries.shape.index(max(entries.shape))
    spots = []
    for shift in (0, 1):
        where = [jax.random.randint(jax.random.fold_in(own_key, axis), (), 0, length) for axis, length in enumerate(entries.shape)]
        where[longest] = (where[longest] + shift) % entries.shape[longest]
        spots.append(tuple(where))
    return entries.at[spots[0]].set(smallest).at[spots[1]].set(top_value)


def level_of(rng, dims, shards, least, largest):
    factor_of = 1.0
    for axis_at, blocks in shards:
        draws = jax.random.uniform(jax.random.fold_in(jax.random.fold_in(rng, 6), axis_at), (blocks,), jnp.float32, least / len(shards), largest / len(shards))
        factor_of = factor_of * jnp.repeat(jnp.exp(draws), dims[axis_at] // blocks).reshape((-1,) + (1,) * (len(dims) - 1 - axis_at))
    return factor_of


def scatter_about(key, extent, scale, reach, shards=(), kind=jnp.bfloat16):
    values = scale * jax.random.normal(key, extent, jnp.float32)
    if shards:
        values = values * level_of(key, extent, shards, -0.22, 0.18)
    return jnp.clip(values, -reach, reach).astype(kind)


def setup_inputs(seed: int = 0) -> dict:
    streams_of = jax.random.split(jax.random.key(seed), 6)
    southward_speed_field = scatter_about(streams_of[0], (VERTICAL_LAYERS, MERIDIONAL_SPANS, ZONAL_POSITIONS), 1.0, 6.0, ((1, 16), (2, 8)))
    thermal_anomaly = scatter_about(streams_of[1], (VERTICAL_LAYERS, MERIDIONAL_SPANS, ZONAL_POSITIONS), 1.0, 6.0, ((1, 16), (2, 8)))
    section_surface = jnp.clip(jnp.exp(math.log(3.0) - 2.3025851 * jax.random.uniform(streams_of[2], (VERTICAL_LAYERS, MERIDIONAL_SPANS, ZONAL_POSITIONS), jnp.float32) ** level_of(streams_of[2], (VERTICAL_LAYERS, MERIDIONAL_SPANS, ZONAL_POSITIONS), ((1, 16), (2, 8)), -0.2, 0.2)), 0.3, 3.0)
    parallel_band_label = draw_parallel_band_label(jax.random.fold_in(streams_of[5], 71), 0)
    ocean_region_label = plant(jax.random.randint(streams_of[4], (MERIDIONAL_SPANS, ZONAL_POSITIONS), 0, 4), jax.random.fold_in(streams_of[4], 1), 0, 3).astype(jnp.int32)
    return dict(southward_speed_field=southward_speed_field, thermal_anomaly=thermal_anomaly, section_surface=section_surface, parallel_band_label=parallel_band_label, ocean_region_label=ocean_region_label)


def reference(southward_speed_field, thermal_anomaly, section_surface, parallel_band_label, ocean_region_label):
    thermal_real_valued = thermal_anomaly.astype(jnp.float32)
    poleward_warmth = jnp.concatenate([thermal_real_valued[:, 1:, :], jnp.zeros_like(thermal_real_valued[:, :1, :])], axis=1)
    interface_warmth = 0.5 * (thermal_real_valued + poleward_warmth)
    thermal_transport = (southward_speed_field.astype(jnp.float32) * interface_warmth * section_surface).astype(jnp.bfloat16)
    levels = thermal_transport.shape[0]
    cell_codes = (ocean_region_label.astype(jnp.int32) * BINS + parallel_band_label.astype(jnp.int32)).reshape(-1)
    flat_flux = thermal_transport.reshape(levels, -1).astype(jnp.float32).T
    bin_sums = jax.ops.segment_sum(flat_flux, cell_codes, num_segments=4 * BINS)
    region_sums = jnp.transpose(bin_sums.reshape(4, BINS, levels), (0, 2, 1))
    regions = jnp.stack([region_sums[0] + region_sums[1] + region_sums[2] + region_sums[3], region_sums[0], region_sums[1] + region_sums[2], region_sums[1], region_sums[2]])
    scale_factor = (BINS / (MERIDIONAL_SPANS * ZONAL_POSITIONS)) ** 0.5
    heat_level = regions * scale_factor
    heat_total = jnp.sum(heat_level, axis=1)
    return heat_level, heat_total
```

```python
import jax
import jax.numpy as jnp
from jax import lax
from jax.experimental import pallas as pl
from jax.experimental.pallas import tpu as pltpu
from jax.sharding import PartitionSpec as P

BINS = 1800
ROWS = 8
LANES = 128
LEVEL_ROWS = 80


def tables_kernel(
    owner_ref, core_ref, v_ref, t_ref, tn_ref, halo_ref, s_ref, bin_ref, reg_ref,
    keep_ref, send_ref, acc_ref, flux_ref,
):
    levels = v_ref.shape[0]
    chunks = v_ref.shape[2] // LANES
    owners = acc_ref.shape[0]
    bins_owned = (BINS + owners - 1) // owners
    step = pl.program_id(0)
    last = pl.num_programs(0) - 1

    @pl.when(step == 0)
    def _():
        acc_ref[...] = jnp.zeros_like(acc_ref)
        flux_ref[:, levels * ROWS :, :] = jnp.zeros(
            (chunks, (LEVEL_ROWS - levels) * ROWS, LANES), jnp.float32
        )

    is_last_row = lax.broadcasted_iota(jnp.int32, (1, ROWS, LANES), 1) == ROWS - 1
    for c in range(chunks):
        cols = slice(c * LANES, (c + 1) * LANES)
        warm = t_ref[:, :, cols].astype(jnp.float32)
        after = tn_ref[:, 0:1, cols].astype(jnp.float32)
        beyond = halo_ref[:, :, cols].astype(jnp.float32)
        after = jnp.where(step == last, beyond, after)
        below = jnp.where(is_last_row, after, pltpu.roll(warm, ROWS - 1, 1))
        face = 0.5 * (warm + below)
        flux = v_ref[:, :, cols].astype(jnp.float32) * face * s_ref[:, :, cols]
        flux_ref[c, : levels * ROWS, :] = flux.reshape(levels * ROWS, LANES)

    slot = lax.broadcasted_iota(jnp.int32, (LANES, LANES), 0)
    nothing = jnp.zeros((LANES, LANES), jnp.bfloat16)

    def one_row(r):
        for p in range(chunks // 2):
            picks = []
            masked = []
            slots = []
            for c in (2 * p, 2 * p + 1):
                own = owner_ref[(step * ROWS + r) * chunks + c]
                picks.append(own)
                cells = flux_ref[c, pl.ds(r, LEVEL_ROWS, stride=ROWS), :].astype(jnp.bfloat16)
                bins = bin_ref[r : r + 1, c * LANES : (c + 1) * LANES] - own * bins_owned
                regs = reg_ref[r : r + 1, c * LANES : (c + 1) * LANES]
                slots.append((slot == bins).astype(jnp.float32).astype(jnp.bfloat16))
                masked.append(
                    [cells * (regs == q).astype(jnp.float32).astype(jnp.bfloat16) for q in range(4)]
                )
            left = jnp.concatenate(
                [jnp.concatenate([masked[0][q], masked[1][q]], axis=1) for q in range(4)], axis=0
            )
            right = jnp.concatenate(
                [
                    jnp.concatenate([slots[0], nothing], axis=1),
                    jnp.concatenate([nothing, slots[1]], axis=1),
                ],
                axis=0,
            )
            sums = lax.dot_general(
                left, right, (((1,), (1,)), ((), ())), preferred_element_type=jnp.float32
            )
            for h in range(2):
                acc_ref[picks[h]] += sums[:, h * LANES : (h + 1) * LANES]

    for r in range(ROWS):
        one_row(r)

    @pl.when(step == last)
    def _():
        core = core_ref[0]
        half = 2 * LEVEL_ROWS
        mine = pl.multiple_of(core * half, half)
        others = pl.multiple_of((1 - core) * half, half)
        for o in range(owners):
            keep_ref[o] = acc_ref[o, pl.ds(mine, half), :]
            send_ref[o] = acc_ref[o, pl.ds(others, half), :].astype(jnp.bfloat16)


def local_tables(owner, core, v, t, halo, s, bins, regs):
    levels, rows, cols = v.shape
    owners = 16
    steps = rows // ROWS
    tile = (levels, ROWS, cols)
    half = 2 * LEVEL_ROWS
    return pl.pallas_call(
        tables_kernel,
        grid_spec=pltpu.PrefetchScalarGridSpec(
            num_scalar_prefetch=2,
            grid=(steps,),
            in_specs=[
                pl.BlockSpec(tile, lambda i, *_: (0, i, 0)),
                pl.BlockSpec(tile, lambda i, *_: (0, i, 0)),
                pl.BlockSpec(tile, lambda i, *_: (0, jnp.minimum(i + 1, steps - 1), 0)),
                pl.BlockSpec((levels, 1, cols), lambda i, *_: (0, 0, 0)),
                pl.BlockSpec(tile, lambda i, *_: (0, i, 0)),
                pl.BlockSpec((ROWS, cols), lambda i, *_: (i, 0)),
                pl.BlockSpec((ROWS, cols), lambda i, *_: (i, 0)),
            ],
            out_specs=[
                pl.BlockSpec((owners, half, LANES), lambda i, *_: (0, 0, 0)),
                pl.BlockSpec((owners, half, LANES), lambda i, *_: (0, 0, 0)),
            ],
            scratch_shapes=[
                pltpu.VMEM((owners, 4 * LEVEL_ROWS, LANES), jnp.float32),
                pltpu.VMEM((cols // LANES, LEVEL_ROWS * ROWS, LANES), jnp.float32),
            ],
        ),
        out_shape=[
            jax.ShapeDtypeStruct((owners, half, LANES), jnp.float32),
            jax.ShapeDtypeStruct((owners, half, LANES), jnp.bfloat16),
        ],
        compiler_params=pltpu.CompilerParams(vmem_limit_bytes=60 * 1024 * 1024),
        name="tables",
    )(owner, core, v, t, t, halo, s, bins, regs)


def assemble_kernel(scale, core_ref, mine_ref, other_ref, level_ref, total_ref):
    owners = mine_ref.shape[0]
    rows = mine_ref.shape[2]
    bins_owned = (BINS + owners - 1) // owners
    step = pl.program_id(0)
    first = core_ref[0] == 0
    lane = lax.broadcasted_iota(jnp.int32, (rows, LANES), 1)

    @pl.when(step == 0)
    def _():
        total_ref[...] = jnp.zeros_like(total_ref)

    def owned(o, q):
        a = mine_ref[o, q % 2].astype(jnp.float32)
        b = other_ref[o, q % 2].astype(jnp.float32)
        return jnp.where(first == (q < 2), a, b)

    tiles = (BINS + LANES - 1) // LANES
    for w in range(tiles):
        start = w * LANES
        width = min(LANES, BINS - start)
        regions = []
        for q in range(4):
            built = None
            for o in range(owners):
                lo = o * bins_owned - start
                if lo >= width or lo + bins_owned <= 0:
                    continue
                part = owned(o, q)
                if lo % LANES:
                    part = pltpu.roll(part, lo % LANES, 1)
                built = part if built is None else jnp.where(lane >= lo, part, built)
            regions.append(built)
        outs = [
            regions[0] + regions[1] + regions[2] + regions[3],
            regions[0],
            regions[1] + regions[2],
            regions[1],
            regions[2],
        ]
        for n in range(5):
            scaled = outs[n] * scale
            level_ref[n, :, start : start + width] = scaled[:, :width]
            total_ref[n : n + 1, start : start + width] += jnp.sum(scaled, axis=0, keepdims=True)[:, :width]


def assemble(core, mine, other, levels, scale):
    owners = mine.shape[0]
    rows = 16
    pieces = pl.BlockSpec((owners, 2, rows, LANES), lambda i, *_: (0, 0, i, 0))
    shape = (owners, 2, LEVEL_ROWS, LANES)

    def body(*refs):
        assemble_kernel(scale, *refs)

    return pl.pallas_call(
        body,
        grid_spec=pltpu.PrefetchScalarGridSpec(
            num_scalar_prefetch=1,
            grid=(LEVEL_ROWS // rows,),
            in_specs=[pieces, pieces],
            out_specs=[
                pl.BlockSpec((5, rows, BINS), lambda i, *_: (0, i, 0)),
                pl.BlockSpec((5, BINS), lambda i, *_: (0, 0)),
            ],
        ),
        out_shape=[
            jax.ShapeDtypeStruct((5, levels, BINS), jnp.float32),
            jax.ShapeDtypeStruct((5, BINS), jnp.float32),
        ],
        name="assemble",
    )(core, mine.reshape(shape), other.reshape(shape))


def shards(v, t, s, bins, regs):
    levels, rows, cols = v.shape
    owners = lax.axis_size("gy")
    count = lax.axis_size("gx")
    bins_owned = (BINS + owners - 1) // owners
    scale = (BINS / (rows * owners * cols * count)) ** 0.5
    core = lax.rem(lax.axis_index("gx"), 2).reshape(1)
    halo = lax.ppermute(t[:, :1, :], "gy", [(k, k - 1) for k in range(1, owners)])
    owner = (bins[:, ::LANES] // bins_owned).reshape(-1)
    keep, send = local_tables(owner, core, v, t, halo, s, bins, regs)
    swap = [(k, k ^ 1) for k in range(count)]
    paired = (keep + lax.ppermute(send, "gx", swap).astype(jnp.float32)).astype(jnp.bfloat16)
    arrived = lax.all_to_all(paired, "gy", 0, 0, tiled=True)
    own = arrived.astype(jnp.float32).sum(axis=0).astype(jnp.bfloat16)
    turned = [
        lax.ppermute(own, "gx", [(k, (k + 2 * d) % count) for k in range(count)]).astype(jnp.float32)
        for d in (1, 2, 3)
    ]
    whole = ((own.astype(jnp.float32) + turned[1]) + (turned[0] + turned[2])).astype(jnp.bfloat16)
    spread = jnp.broadcast_to(whole[None], (owners, *whole.shape))
    mine = lax.all_to_all(spread, "gy", 0, 0, tiled=True)
    other = lax.ppermute(mine, "gx", swap)
    return tuple(assemble(core, mine, other, levels, scale))


def solution(mesh):
    return jax.shard_map(
        shards,
        mesh=mesh,
        in_specs=(
            P(None, "gy", "gx"),
            P(None, "gy", "gx"),
            P(None, "gy", "gx"),
            P("gy", "gx"),
            P("gy", "gx"),
        ),
        out_specs=(P(), P()),
        check_vma=False,
    )
```

```python
import jax
import jax.numpy as jnp
from jax import lax
from jax.experimental import pallas as pl
from jax.experimental.pallas import tpu as pltpu
from jax.sharding import PartitionSpec as P

BINS = 1800
ROWS = 8
LANES = 128
LEVEL_ROWS = 80
PAIR_SLOTS = 136
UNROLL = 8
BF16 = jnp.bfloat16
F32 = jnp.float32


def owner_of(bins, owned):
    factor = (1 << 16) // owned + 1
    return lax.shift_right_logical(bins * factor, 16)


def check_owner_rule(owned):
    factor = (1 << 16) // owned + 1
    assert all((b * factor) >> 16 == b // owned for b in range(BINS))


def runs_kernel(
    owned, v_ref, t_ref, s_ref, bin_ref, reg_ref, first_ref,
    runs_ref, tags_ref, edge_ref, pairs_ref,
    flux_ref, carry_ref, open_ref, used_ref,
):
    levels = v_ref.shape[0]
    chunks = v_ref.shape[2] // LANES
    spare = runs_ref.shape[0] - 1
    step = pl.program_id(0)
    block = pl.num_programs(0) - 1 - step
    filled = levels * ROWS
    owners_at = 2 * PAIR_SLOTS
    edge_at = owners_at + PAIR_SLOTS

    @pl.when(step == 0)
    def _():
        carry_ref[...] = jnp.zeros_like(carry_ref)
        flux_ref[:, filled:, :] = jnp.zeros((chunks, LEVEL_ROWS * ROWS - filled, LANES), F32)
        runs_ref[spare] = jnp.zeros((LEVEL_ROWS, LANES), BF16)
        tags_ref[spare, 0] = jnp.full((16, LANES), -1, BF16)
        tags_ref[spare, 1] = jnp.zeros((16, LANES), BF16)
        used_ref[0] = 0

        def clear_pair(n, _):
            pairs_ref[2 * n] = spare
            pairs_ref[2 * n + 1] = spare
            pairs_ref[owners_at + n] = 0
            return 0

        lax.fori_loop(0, PAIR_SLOTS, clear_pair, 0)
        for o in range(16):
            open_ref[o] = -1
        for c in range(chunks):
            cols = slice(c * LANES, (c + 1) * LANES)
            for n, ref in enumerate((t_ref, v_ref, s_ref)):
                flux_ref[c, :filled, :] = ref[:, :, cols].astype(F32).reshape(filled, LANES)
                edge_ref[n, c] = flux_ref[c, pl.ds(ROWS - 1, LEVEL_ROWS, stride=ROWS), :]

    is_last_row = lax.broadcasted_iota(jnp.int32, (1, ROWS, LANES), 1) == ROWS - 1
    for c in range(chunks):
        cols = slice(c * LANES, (c + 1) * LANES)
        warm = t_ref[:, :, cols].astype(F32)
        rolled = pltpu.roll(warm, ROWS - 1, 1)
        below = jnp.where(is_last_row, carry_ref[:, :, cols], rolled)
        carry_ref[:, :, cols] = rolled
        flux = v_ref[:, :, cols].astype(F32) * (warm + below) * s_ref[:, :, cols]
        flux_ref[c, :filled, :] = flux.reshape(filled, LANES)
        for r in range(ROWS):
            cells = flux_ref[c, pl.ds(r, LEVEL_ROWS, stride=ROWS), :]
            runs_ref[(block * ROWS + r) * chunks + c] = cells.astype(BF16)

    bins = bin_ref[...]
    regs = reg_ref[...]
    code = bins - owner_of(bins, owned) * owned + (regs & 1) * LANES
    code = code.astype(F32)
    high = lax.shift_right_logical(regs, 1).astype(F32)
    for r in range(ROWS):
        for c in range(chunks):
            cols = slice(c * LANES, (c + 1) * LANES)
            run = (block * ROWS + r) * chunks + c
            tags_ref[run, 0] = jnp.broadcast_to(code[r : r + 1, cols], (16, LANES)).astype(BF16)
            tags_ref[run, 1] = jnp.broadcast_to(high[r : r + 1, cols], (16, LANES)).astype(BF16)

    def enlist(r, c):
        own = owner_of(first_ref[r, c * LANES], owned)
        held = open_ref[own]
        used = used_ref[0]
        is_open = held >= 0
        pair = jnp.where(is_open, held, used)
        pairs_ref[2 * pair + jnp.where(is_open, 1, 0)] = (block * ROWS + r) * chunks + c
        pairs_ref[owners_at + pair] = own
        open_ref[own] = jnp.where(is_open, -1, used)
        used_ref[0] = used + jnp.where(is_open, 0, 1)

    for r in range(ROWS - 1):
        for c in range(chunks):
            enlist(r, c)

    @pl.when(step > 0)
    def _():
        for c in range(chunks):
            enlist(ROWS - 1, c)

    @pl.when(step == 0)
    def _():
        for c in range(chunks):
            pairs_ref[edge_at + c] = owner_of(first_ref[ROWS - 1, c * LANES], owned)

    pairs_ref[edge_at + chunks] = used_ref[0]


def sums_kernel(
    pairs_ref, core_ref, halo_ref, runs_ref, tags_ref, edge_ref,
    keep_ref, send_ref, acc_ref, halo32_ref,
):
    levels, cols = halo_ref.shape
    chunks = cols // LANES
    spare = runs_ref.shape[0] - 1
    owners = acc_ref.shape[0]
    owners_at = 2 * PAIR_SLOTS
    edge_at = owners_at + PAIR_SLOTS
    acc_ref[...] = jnp.zeros_like(acc_ref)
    halo32_ref[:levels] = halo_ref[...].astype(F32)
    halo32_ref[levels:] = jnp.zeros((LEVEL_ROWS - levels, cols), F32)
    slot = lax.broadcasted_iota(jnp.int32, (2 * LANES, LANES), 0).astype(F32).astype(BF16)
    one = jnp.ones((2 * LANES, LANES), BF16)
    nothing = jnp.zeros((2 * LANES, LANES), BF16)

    def stacked(x, n):
        return jnp.concatenate([x] * n, axis=0)

    def add_pair(own, firsts, run_a, run_b):
        lows, highs, spots = [], [], []
        for cells, run in zip(firsts, (run_a, run_b)):
            upper = cells * stacked(tags_ref[run, 1], LEVEL_ROWS // 16)
            lows.append(cells - upper)
            highs.append(upper)
            spots.append(jnp.where(slot == stacked(tags_ref[run, 0], 2 * LANES // 16), one, nothing))
        left = jnp.concatenate(
            [jnp.concatenate(lows, axis=1), jnp.concatenate(highs, axis=1)], axis=0
        )
        right = jnp.concatenate(spots, axis=1)
        acc_ref[own] += lax.dot_general(
            left, right, (((1,), (1,)), ((), ())), preferred_element_type=F32
        )

    def several(n, _):
        for u in range(UNROLL):
            pair = n * UNROLL + u
            a = pairs_ref[2 * pair]
            b = pairs_ref[2 * pair + 1]
            add_pair(pairs_ref[owners_at + pair], (runs_ref[a], runs_ref[b]), a, b)
        return 0

    used = pairs_ref[edge_at + chunks]
    lax.fori_loop(0, lax.div(used + UNROLL - 1, UNROLL), several, 0)

    for c in range(chunks):
        warm = edge_ref[0, c] + halo32_ref[:, c * LANES : (c + 1) * LANES]
        flux = (edge_ref[1, c] * warm * edge_ref[2, c]).astype(BF16)
        add_pair(
            pairs_ref[edge_at + c], (flux, runs_ref[spare]), spare - chunks + c, spare
        )

    core = core_ref[0]
    mine = pl.multiple_of(core * LEVEL_ROWS, LEVEL_ROWS)
    others = pl.multiple_of((1 - core) * LEVEL_ROWS, LEVEL_ROWS)
    for o in range(owners):
        keep_ref[o] = acc_ref[o, pl.ds(mine, LEVEL_ROWS), :]
        send_ref[o] = acc_ref[o, pl.ds(others, LEVEL_ROWS), :].astype(BF16)


def local_runs(v, t, s, bins, regs, owned):
    levels, rows, cols = v.shape
    steps = rows // ROWS
    chunks = cols // LANES
    count = rows * chunks
    tile = pl.BlockSpec((levels, ROWS, cols), lambda i: (0, steps - 1 - i, 0))
    flat = pl.BlockSpec((ROWS, cols), lambda i: (steps - 1 - i, 0))
    flat_scalar = pl.BlockSpec((ROWS, cols), lambda i: (steps - 1 - i, 0), memory_space=pltpu.SMEM)
    vmem = pl.BlockSpec(memory_space=pltpu.VMEM)

    def body(*refs):
        runs_kernel(owned, *refs)

    return pl.pallas_call(
        body,
        grid=(steps,),
        in_specs=[tile, tile, tile, flat, flat, flat_scalar],
        out_specs=[vmem, vmem, vmem, pl.BlockSpec(memory_space=pltpu.SMEM)],
        out_shape=[
            pltpu.VMEM((count + 1, LEVEL_ROWS, LANES), BF16),
            pltpu.VMEM((count + 1, 2, 16, LANES), BF16),
            pltpu.VMEM((3, chunks, LEVEL_ROWS, LANES), F32),
            jax.ShapeDtypeStruct((3 * PAIR_SLOTS + chunks + 1,), jnp.int32),
        ],
        scratch_shapes=[
            pltpu.VMEM((chunks, LEVEL_ROWS * ROWS, LANES), F32),
            pltpu.VMEM((levels, ROWS, cols), F32),
            pltpu.SMEM((16,), jnp.int32),
            pltpu.SMEM((1,), jnp.int32),
        ],
        compiler_params=pltpu.CompilerParams(vmem_limit_bytes=40 * 1024 * 1024),
        name="runs",
    )(v, t, s, bins, regs, bins)


def in_vmem(x):
    return pltpu.with_memory_space_constraint(x, pltpu.VMEM)


def local_sums(pairs, core, halo, runs, tags, edge):
    owners = 16
    smem = pl.BlockSpec(memory_space=pltpu.SMEM)
    vmem = pl.BlockSpec(memory_space=pltpu.VMEM)
    return pl.pallas_call(
        sums_kernel,
        in_specs=[smem, smem, vmem, vmem, vmem, vmem],
        out_specs=[vmem, vmem],
        out_shape=[
            pltpu.VMEM((owners, LEVEL_ROWS, 2 * LANES), F32),
            pltpu.VMEM((owners, LEVEL_ROWS, 2 * LANES), BF16),
        ],
        scratch_shapes=[
            pltpu.VMEM((owners, 2 * LEVEL_ROWS, 2 * LANES), F32),
            pltpu.VMEM((LEVEL_ROWS, halo.shape[1]), F32),
        ],
        compiler_params=pltpu.CompilerParams(vmem_limit_bytes=40 * 1024 * 1024),
        name="sums",
    )(pairs, core, in_vmem(halo), in_vmem(runs), in_vmem(tags), in_vmem(edge))


def assemble_kernel(scale, core_ref, mine_ref, other_ref, level_ref, total_ref):
    owners = mine_ref.shape[0]
    rows = level_ref.shape[1]
    owned = (BINS + owners - 1) // owners
    step = pl.program_id(0)
    first = core_ref[0] == 0
    lane = lax.broadcasted_iota(jnp.int32, (rows, LANES), 1)
    here = pl.ds(pl.multiple_of(step * rows, rows), rows)

    @pl.when(step == 0)
    def _():
        total_ref[...] = jnp.zeros_like(total_ref)

    def piece(o, q):
        side = slice((q % 2) * LANES, (q % 2 + 1) * LANES)
        a = mine_ref[o, here, side].astype(F32)
        b = other_ref[o, here, side].astype(F32)
        return jnp.where(first == (q < 2), a, b)

    tiles = (BINS + LANES - 1) // LANES
    for w in range(tiles):
        start = w * LANES
        width = min(LANES, BINS - start)
        regions = []
        for q in range(4):
            built = None
            for o in range(owners):
                lo = o * owned - start
                if lo >= width or lo + owned <= 0:
                    continue
                part = piece(o, q)
                if lo % LANES:
                    part = pltpu.roll(part, lo % LANES, 1)
                built = part if built is None else jnp.where(lane >= lo, part, built)
            regions.append(built)
        outs = [
            regions[0] + regions[1] + regions[2] + regions[3],
            regions[0],
            regions[1] + regions[2],
            regions[1],
            regions[2],
        ]
        for n in range(5):
            scaled = outs[n] * scale
            level_ref[n, :, start : start + width] = scaled[:, :width]
            total_ref[n : n + 1, start : start + width] += jnp.sum(
                scaled, axis=0, keepdims=True
            )[:, :width]


def assemble(core, mine, other, levels, scale):
    rows = 16
    vmem = pl.BlockSpec(memory_space=pltpu.VMEM)

    def body(*refs):
        assemble_kernel(scale, *refs)

    return pl.pallas_call(
        body,
        grid=(LEVEL_ROWS // rows,),
        in_specs=[pl.BlockSpec(memory_space=pltpu.SMEM), vmem, vmem],
        out_specs=[
            pl.BlockSpec((5, rows, BINS), lambda i: (0, i, 0)),
            pl.BlockSpec((5, BINS), lambda i: (0, 0)),
        ],
        out_shape=[
            jax.ShapeDtypeStruct((5, levels, BINS), F32),
            jax.ShapeDtypeStruct((5, BINS), F32),
        ],
        name="assemble",
    )(core, in_vmem(mine), in_vmem(other))


def shards(v, t, s, bins, regs):
    levels, rows, cols = v.shape
    owners = lax.axis_size("gy")
    count = lax.axis_size("gx")
    owned = (BINS + owners - 1) // owners
    check_owner_rule(owned)
    scale = 0.5 * (BINS / (rows * owners * cols * count)) ** 0.5
    core = lax.rem(lax.axis_index("gx"), 2).reshape(1)

    def swapped(x, bit):
        return lax.ppermute(x, "gx", [(k, k ^ bit) for k in range(count)])

    halo = lax.ppermute(t[:, 0, :], "gy", [(k, k - 1) for k in range(1, owners)])
    runs, tags, edge, pairs = local_runs(v, t, s, bins, regs, owned)
    keep, send = local_sums(pairs, core, halo, runs, tags, edge)
    paired = (keep + swapped(send, 1).astype(F32)).astype(BF16)
    arrived = lax.all_to_all(paired, "gy", 0, 0, tiled=True)
    whole = arrived.astype(F32).sum(axis=0).astype(BF16)
    for bit in (2, 6):
        whole = (whole.astype(F32) + swapped(whole, bit).astype(F32)).astype(BF16)
    spread = jnp.broadcast_to(whole[None], (owners, *whole.shape))
    mine = lax.all_to_all(spread, "gy", 0, 0, tiled=True)
    other = swapped(mine, 1)
    return tuple(assemble(core, mine, other, levels, scale))


def solution(mesh):
    return jax.shard_map(
        shards,
        mesh=mesh,
        in_specs=(
            P(None, "gy", "gx"),
            P(None, "gy", "gx"),
            P(None, "gy", "gx"),
            P("gy", "gx"),
            P("gy", "gx"),
        ),
        out_specs=(P(), P()),
        check_vma=False,
    )
```

```python
import jax
import jax.numpy as jnp
from jax import lax
from jax.experimental import pallas as pl
from jax.experimental.pallas import tpu as pltpu
from jax.sharding import PartitionSpec as P

BINS = 1800
ROWS = 8
LANES = 128
LEVEL_ROWS = 80
GROUP = 4
GROUPS = 75
UNROLL = 5
OWNERS_AT = GROUP * GROUPS
TRASH_AT = OWNERS_AT + GROUPS
EDGE_AT = TRASH_AT + 2
BF16 = jnp.bfloat16
F32 = jnp.float32


def owner_of(bins, owned):
    factor = (1 << 16) // owned + 1
    return lax.shift_right_logical(bins * factor, 16)


def check_owner_rule(owned):
    factor = (1 << 16) // owned + 1
    assert all((b * factor) >> 16 == b // owned for b in range(BINS))


def runs_kernel(
    owned, v_ref, t_ref, s_ref, bin_ref, reg_ref, first_ref,
    runs_ref, tags_ref, edge_ref, edge_tags_ref, halo_ref, lists_ref,
    flux_ref, carry_ref, open_ref, used_ref,
):
    levels = v_ref.shape[0]
    chunks = v_ref.shape[2] // LANES
    spare = runs_ref.shape[0] - 1
    step = pl.program_id(0)
    last = pl.num_programs(0) - 1
    block = last - step
    filled = levels * ROWS

    @pl.when(step == 0)
    def _():
        carry_ref[...] = jnp.zeros_like(carry_ref)
        flux_ref[:, filled:, :] = jnp.zeros((chunks, LEVEL_ROWS * ROWS - filled, LANES), F32)
        runs_ref[spare] = jnp.zeros((LEVEL_ROWS, LANES), BF16)
        tags_ref[spare, 0] = jnp.full((16, LANES), -1, BF16)
        tags_ref[spare, 1] = jnp.zeros((16, LANES), BF16)
        used_ref[0] = 0

        def clear(n, _):
            for k in range(GROUP):
                lists_ref[GROUP * n + k] = spare
            lists_ref[OWNERS_AT + n] = 0
            return 0

        lax.fori_loop(0, GROUPS, clear, 0)
        for o in range(17):
            open_ref[o] = -1
        for c in range(chunks):
            cols = slice(c * LANES, (c + 1) * LANES)
            for n, ref in enumerate((t_ref, v_ref, s_ref)):
                for k in range(0, levels, 5):
                    part = ref[k : k + 5, :, cols].astype(F32)
                    flux_ref[c, k * ROWS : (k + 5) * ROWS, :] = part.reshape(5 * ROWS, LANES)
                edge_ref[n, c] = flux_ref[c, pl.ds(ROWS - 1, LEVEL_ROWS, stride=ROWS), :]

    def enlist(r, c):
        live = True if r < ROWS - 1 else step > 0
        own = owner_of(first_ref[r, c * LANES], owned)
        if r == ROWS - 1:
            lists_ref[jnp.where(live, TRASH_AT + 1, EDGE_AT + c)] = own
        key = own if r < ROWS - 1 else jnp.where(live, own, 16)
        held = open_ref[key]
        used = used_ref[0]
        is_open = held >= 0
        spot = jnp.where(is_open, held, GROUP * used)
        if r == ROWS - 1:
            lists_ref[jnp.where(live, spot, TRASH_AT)] = (block * ROWS + r) * chunks + c
            lists_ref[jnp.where(live, OWNERS_AT + spot // GROUP, TRASH_AT)] = own
            open_ref[key] = jnp.where(live & ((spot + 1) % GROUP != 0), spot + 1, -1)
            used_ref[0] = used + jnp.where(live & ~is_open, 1, 0)
        else:
            lists_ref[spot] = (block * ROWS + r) * chunks + c
            lists_ref[OWNERS_AT + lax.shift_right_logical(spot, 2)] = own
            open_ref[key] = jnp.where(((spot + 1) & (GROUP - 1)) != 0, spot + 1, -1)
            used_ref[0] = used + jnp.where(is_open, 0, 1)

    waiting = [(r, c) for r in range(ROWS) for c in range(chunks)]
    is_last_row = lax.broadcasted_iota(jnp.int32, (1, ROWS, LANES), 1) == ROWS - 1
    for c in range(chunks):
        cols = slice(c * LANES, (c + 1) * LANES)
        for k in range(0, levels, 5):
            here = slice(k, k + 5)
            flat = slice(k * ROWS, (k + 5) * ROWS)
            warm = t_ref[here, :, cols].astype(F32)
            rolled = pltpu.roll(warm, ROWS - 1, 1)
            carried = carry_ref[c, flat, :].reshape(5, ROWS, LANES)
            below = jnp.where(is_last_row, carried, rolled)
            carry_ref[c, flat, :] = rolled.reshape(5 * ROWS, LANES)
            flux = v_ref[here, :, cols].astype(F32) * (warm + below) * s_ref[here, :, cols]
            flux_ref[c, flat, :] = flux.reshape(5 * ROWS, LANES)
            if waiting:
                enlist(*waiting.pop(0))
        for r in range(ROWS):
            cells = flux_ref[c, pl.ds(r, LEVEL_ROWS, stride=ROWS), :]
            runs_ref[(block * ROWS + r) * chunks + c] = cells.astype(BF16)

    bins = bin_ref[...]
    regs = reg_ref[...]
    code = bins - owner_of(bins, owned) * owned + (regs & 1) * LANES
    code = code.astype(F32)
    high = lax.shift_right_logical(regs, 1).astype(F32)
    for r in range(ROWS):
        for c in range(chunks):
            cols = slice(c * LANES, (c + 1) * LANES)
            run = (block * ROWS + r) * chunks + c
            tags_ref[run, 0] = jnp.broadcast_to(code[r : r + 1, cols], (16, LANES)).astype(BF16)
            tags_ref[run, 1] = jnp.broadcast_to(high[r : r + 1, cols], (16, LANES)).astype(BF16)

    @pl.when(step == 0)
    def _():
        edge_tags_ref[...] = tags_ref[spare - chunks : spare]

    @pl.when(step == last)
    def _():
        lists_ref[EDGE_AT + chunks] = used_ref[0]
        for c in range(chunks):
            row = carry_ref[c, pl.ds(ROWS - 1, LEVEL_ROWS, stride=ROWS), :]
            halo_ref[:, c * LANES : (c + 1) * LANES] = row.astype(BF16)


def stacked(x, n):
    return jnp.concatenate([x] * n, axis=0)


def group_sums(slot, tags_ref, members):
    lows, highs, spots = [], [], []
    one = jnp.ones((2 * LANES, LANES), BF16)
    nothing = jnp.zeros((2 * LANES, LANES), BF16)
    for cells, run in members:
        upper = cells * stacked(tags_ref[run, 1], LEVEL_ROWS // 16)
        lows.append(cells - upper)
        highs.append(upper)
        spots.append(jnp.where(slot == stacked(tags_ref[run, 0], 2 * LANES // 16), one, nothing))
    left = jnp.concatenate([jnp.concatenate(lows, axis=1), jnp.concatenate(highs, axis=1)], axis=0)
    right = jnp.concatenate(spots, axis=1)
    return lax.dot_general(left, right, (((1,), (1,)), ((), ())), preferred_element_type=F32)


def slots():
    return lax.broadcasted_iota(jnp.int32, (2 * LANES, LANES), 0).astype(F32).astype(BF16)


def sums_kernel(lists_ref, runs_ref, tags_ref, acc_ref):
    acc_ref[...] = jnp.zeros_like(acc_ref)
    slot = slots()
    chunks = lists_ref.shape[0] - EDGE_AT - 3

    def several(n, _):
        for u in range(UNROLL):
            group = n * UNROLL + u
            names = [lists_ref[GROUP * group + k] for k in range(GROUP)]
            own = lists_ref[OWNERS_AT + group]
            acc_ref[own] += group_sums(slot, tags_ref, [(runs_ref[a], a) for a in names])
        return 0

    used = lists_ref[EDGE_AT + chunks]
    lax.fori_loop(0, lax.div(used + UNROLL - 1, UNROLL), several, 0)


def edge_kernel(
    lists_ref, core_ref, halo_ref, tags_ref, edge_ref, sums_ref,
    acc_ref, keep_ref, send_ref,
):
    del sums_ref
    chunks = halo_ref.shape[1] // LANES
    owners = acc_ref.shape[0]
    slot = slots()
    for c in range(chunks):
        halo = halo_ref[:, c * LANES : (c + 1) * LANES].astype(F32)
        flux = (edge_ref[1, c] * (edge_ref[0, c] + halo) * edge_ref[2, c]).astype(BF16)
        acc_ref[lists_ref[EDGE_AT + c]] += group_sums(slot, tags_ref, [(flux, c)])
    core = core_ref[0]
    mine = pl.multiple_of(core * LEVEL_ROWS, LEVEL_ROWS)
    others = pl.multiple_of((1 - core) * LEVEL_ROWS, LEVEL_ROWS)
    for o in range(owners):
        keep_ref[o] = acc_ref[o, pl.ds(mine, LEVEL_ROWS), :]
        send_ref[o] = acc_ref[o, pl.ds(others, LEVEL_ROWS), :].astype(BF16)


def in_vmem(x):
    return pltpu.with_memory_space_constraint(x, pltpu.VMEM)


def in_hbm(x):
    return pltpu.with_memory_space_constraint(x, pltpu.HBM)


SMEM_WHOLE = pl.BlockSpec(memory_space=pltpu.SMEM)
VMEM_WHOLE = pl.BlockSpec(memory_space=pltpu.VMEM)


def local_runs(v, t, s, bins, regs, owned):
    levels, rows, cols = v.shape
    steps = rows // ROWS
    chunks = cols // LANES
    count = rows * chunks
    tile = pl.BlockSpec((levels, ROWS, cols), lambda i: (0, steps - 1 - i, 0))
    flat = pl.BlockSpec((ROWS, cols), lambda i: (steps - 1 - i, 0))
    flat_scalar = pl.BlockSpec((ROWS, cols), lambda i: (steps - 1 - i, 0), memory_space=pltpu.SMEM)

    def body(*refs):
        runs_kernel(owned, *refs)

    v, t, s, bins, regs = (in_hbm(x) for x in (v, t, s, bins, regs))
    return pl.pallas_call(
        body,
        grid=(steps,),
        in_specs=[tile, tile, tile, flat, flat, flat_scalar],
        out_specs=[VMEM_WHOLE] * 5 + [SMEM_WHOLE],
        out_shape=[
            pltpu.VMEM((count + 1, LEVEL_ROWS, LANES), BF16),
            pltpu.VMEM((count + 1, 2, 16, LANES), BF16),
            pltpu.VMEM((3, chunks, LEVEL_ROWS, LANES), F32),
            pltpu.VMEM((chunks, 2, 16, LANES), BF16),
            pltpu.VMEM((LEVEL_ROWS, cols), BF16),
            jax.ShapeDtypeStruct((EDGE_AT + chunks + 3,), jnp.int32),
        ],
        scratch_shapes=[
            pltpu.VMEM((chunks, LEVEL_ROWS * ROWS, LANES), F32),
            pltpu.VMEM((chunks, LEVEL_ROWS * ROWS, LANES), F32),
            pltpu.SMEM((17,), jnp.int32),
            pltpu.SMEM((1,), jnp.int32),
        ],
        compiler_params=pltpu.CompilerParams(vmem_limit_bytes=16 * 1024 * 1024),
        name="runs", cost_estimate=pl.CostEstimate(flops=4000000000, bytes_accessed=20000000, transcendentals=0),
    )(v, t, s, bins, regs, bins)


def local_sums(lists, runs, tags):
    return pl.pallas_call(
        sums_kernel,
        in_specs=[SMEM_WHOLE, VMEM_WHOLE, VMEM_WHOLE],
        out_specs=VMEM_WHOLE,
        out_shape=pltpu.VMEM((16, 2 * LEVEL_ROWS, 2 * LANES), F32),
        compiler_params=pltpu.CompilerParams(vmem_limit_bytes=8 * 1024 * 1024),
        name="sums", cost_estimate=pl.CostEstimate(flops=4000000000, bytes_accessed=1000, transcendentals=0),
    )(lists, in_vmem(runs), in_vmem(tags))


def edge_sums(lists, core, halo, tags, edge, sums):
    owners = sums.shape[0]
    return pl.pallas_call(
        edge_kernel,
        in_specs=[SMEM_WHOLE, SMEM_WHOLE] + [VMEM_WHOLE] * 4,
        out_specs=[VMEM_WHOLE] * 3,
        out_shape=[
            pltpu.VMEM(sums.shape, F32),
            pltpu.VMEM((owners, LEVEL_ROWS, 2 * LANES), F32),
            pltpu.VMEM((owners, LEVEL_ROWS, 2 * LANES), BF16),
        ],
        input_output_aliases={5: 0},
        compiler_params=pltpu.CompilerParams(vmem_limit_bytes=8 * 1024 * 1024),
        name="edge",
    )(lists, core, in_vmem(halo), in_vmem(tags), in_vmem(edge), in_vmem(sums))[1:]


def assemble_kernel(scale, core_ref, mine_ref, other_ref, level_ref, total_ref):
    owners = mine_ref.shape[0]
    rows = level_ref.shape[1]
    owned = (BINS + owners - 1) // owners
    step = pl.program_id(0)
    first = core_ref[0] == 0
    lane = lax.broadcasted_iota(jnp.int32, (rows, LANES), 1)
    here = pl.ds(pl.multiple_of(step * rows, rows), rows)

    @pl.when(step == 0)
    def _():
        total_ref[...] = jnp.zeros_like(total_ref)

    def piece(o, q):
        side = slice((q % 2) * LANES, (q % 2 + 1) * LANES)
        a = mine_ref[o, here, side].astype(F32)
        b = other_ref[o, here, side].astype(F32)
        return jnp.where(first == (q < 2), a, b)

    tiles = (BINS + LANES - 1) // LANES
    for w in range(tiles):
        start = w * LANES
        width = min(LANES, BINS - start)
        regions = []
        for q in range(4):
            built = None
            for o in range(owners):
                lo = o * owned - start
                if lo >= width or lo + owned <= 0:
                    continue
                part = piece(o, q)
                if lo % LANES:
                    part = pltpu.roll(part, lo % LANES, 1)
                built = part if built is None else jnp.where(lane >= lo, part, built)
            regions.append(built)
        outs = [
            regions[0] + regions[1] + regions[2] + regions[3],
            regions[0],
            regions[1] + regions[2],
            regions[1],
            regions[2],
        ]
        for n in range(5):
            scaled = outs[n] * scale
            level_ref[n, :, start : start + width] = scaled[:, :width]
            total_ref[n : n + 1, start : start + width] += jnp.sum(
                scaled, axis=0, keepdims=True
            )[:, :width]


def assemble(core, mine, other, levels, scale):
    rows = 16
    vmem = pl.BlockSpec(memory_space=pltpu.VMEM)

    def body(*refs):
        assemble_kernel(scale, *refs)

    return pl.pallas_call(
        body,
        grid=(LEVEL_ROWS // rows,),
        in_specs=[pl.BlockSpec(memory_space=pltpu.SMEM), vmem, vmem],
        out_specs=[
            pl.BlockSpec((5, rows, BINS), lambda i: (0, i, 0)),
            pl.BlockSpec((5, BINS), lambda i: (0, 0)),
        ],
        out_shape=[
            jax.ShapeDtypeStruct((5, levels, BINS), F32),
            jax.ShapeDtypeStruct((5, BINS), F32),
        ],
        name="assemble",
    )(core, in_vmem(mine), in_vmem(other))


def shards(v, t, s, bins, regs):
    levels, rows, cols = v.shape
    owners = lax.axis_size("gy")
    count = lax.axis_size("gx")
    owned = (BINS + owners - 1) // owners
    check_owner_rule(owned)
    scale = 0.5 * (BINS / (rows * owners * cols * count)) ** 0.5
    core = lax.rem(lax.axis_index("gx"), 2).reshape(1)

    def swapped(x, bit):
        return lax.ppermute(x, "gx", [(k, k ^ bit) for k in range(count)])

    runs, tags, edge, edge_tags, first_row, lists = local_runs(v, t, s, bins, regs, owned)
    halo = lax.ppermute(first_row, "gy", [(k, k - 1) for k in range(1, owners)])
    sums = local_sums(lists, runs, tags)
    keep, send = edge_sums(lists, core, halo, edge_tags, edge, sums)
    paired = (keep + swapped(send, 1).astype(F32)).astype(BF16)
    arrived = lax.all_to_all(paired, "gy", 0, 0, tiled=True)
    whole = arrived.astype(F32).sum(axis=0).astype(BF16)
    for bit in (2, 6):
        whole = (whole.astype(F32) + swapped(whole, bit).astype(F32)).astype(BF16)
    spread = jnp.broadcast_to(whole[None], (owners, *whole.shape))
    mine = lax.all_to_all(spread, "gy", 0, 0, tiled=True)
    other = swapped(mine, 1)
    return tuple(assemble(core, mine, other, levels, scale))


def solution(mesh):
    return jax.shard_map(
        shards,
        mesh=mesh,
        in_specs=(
            P(None, "gy", "gx"),
            P(None, "gy", "gx"),
            P(None, "gy", "gx"),
            P("gy", "gx"),
            P("gy", "gx"),
        ),
        out_specs=(P(), P()),
        check_vma=False,
    )
```

```python
import jax
import jax.numpy as jnp
from jax import lax
from jax.experimental import pallas as pl
from jax.experimental.pallas import tpu as pltpu
from jax.sharding import PartitionSpec as P

BINS = 1800
ROWS = 8
PITCH = 9
AHEAD = 3
LANES = 128
LEVEL_ROWS = 80
GROUP = 4
GROUPS = 75
UNROLL = 5
OWNERS_AT = GROUP * GROUPS
TRASH_AT = OWNERS_AT + GROUPS
EDGE_AT = TRASH_AT + 2
BF16 = jnp.bfloat16
F32 = jnp.float32


def owner_of(bins, owned):
    factor = (1 << 16) // owned + 1
    return lax.shift_right_logical(bins * factor, 16)


def check_owner_rule(owned):
    factor = (1 << 16) // owned + 1
    assert all((b * factor) >> 16 == b // owned for b in range(BINS))


def runs_kernel(
    owned, v_hbm, t_hbm, s_hbm, bin_ref, reg_ref, first_ref,
    runs_ref, tags_ref, edge_ref, edge_tags_ref, halo_ref, lists_ref,
    v_all, t_all, s_all, flux_ref, carry_ref, open_ref, used_ref, sem_ref,
):
    steps, levels = v_all.shape[:2]
    chunks = v_all.shape[3] // LANES
    spare = runs_ref.shape[0] - 1
    step = pl.program_id(0)
    last = steps - 1
    block = last - step
    v_ref, t_ref, s_ref = v_all.at[step], t_all.at[step], s_all.at[step]

    def copies(i):
        rows = pl.ds(pl.multiple_of((last - i) * ROWS, ROWS), ROWS)
        return [
            pltpu.make_async_copy(far.at[:, rows, :], near.at[i], sem_ref.at[n, i])
            for n, (far, near) in enumerate(((t_hbm, t_all), (v_hbm, v_all), (s_hbm, s_all)))
        ]

    @pl.when(step == 0)
    def _():
        for i in range(AHEAD):
            for copy in copies(i):
                copy.start()

        carry_ref[...] = jnp.zeros_like(carry_ref)
        flux_ref[...] = jnp.zeros_like(flux_ref)
        runs_ref[spare] = jnp.zeros((LEVEL_ROWS, LANES), BF16)
        tags_ref[spare, 0] = jnp.full((16, LANES), -1, BF16)
        tags_ref[spare, 1] = jnp.zeros((16, LANES), BF16)
        used_ref[0] = 0

        for n in range(OWNERS_AT):
            lists_ref[n] = spare
        for n in range(OWNERS_AT, TRASH_AT):
            lists_ref[n] = 0
        for o in range(17):
            open_ref[o] = -1

    for copy in copies(step):
        copy.wait()

    @pl.when(step < steps - AHEAD)
    def _():
        for copy in copies(step + AHEAD):
            copy.start()

    @pl.when(step == 0)
    def _():
        for c in range(chunks):
            cols = slice(c * LANES, (c + 1) * LANES)
            for n, ref in enumerate((t_ref, v_ref, s_ref)):
                for k in range(levels):
                    flux_ref[c, k * PITCH : k * PITCH + ROWS, :] = ref[k, :, cols].astype(F32)
                edge_ref[n, c] = flux_ref[c, pl.ds(ROWS - 1, LEVEL_ROWS, stride=PITCH), :]

    def enlist(r, c):
        live = True if r < ROWS - 1 else step > 0
        own = owner_of(first_ref[r, c * LANES], owned)
        if r == ROWS - 1:
            lists_ref[jnp.where(live, TRASH_AT + 1, EDGE_AT + c)] = own
        key = own if r < ROWS - 1 else jnp.where(live, own, 16)
        held = open_ref[key]
        used = used_ref[0]
        is_open = held >= 0
        spot = jnp.where(is_open, held, GROUP * used)
        if r == ROWS - 1:
            lists_ref[jnp.where(live, spot, TRASH_AT)] = (block * ROWS + r) * chunks + c
            lists_ref[jnp.where(live, OWNERS_AT + spot // GROUP, TRASH_AT)] = own
            open_ref[key] = jnp.where(live & ((spot + 1) % GROUP != 0), spot + 1, -1)
            used_ref[0] = used + jnp.where(live & ~is_open, 1, 0)
        else:
            lists_ref[spot] = (block * ROWS + r) * chunks + c
            lists_ref[OWNERS_AT + lax.shift_right_logical(spot, 2)] = own
            open_ref[key] = jnp.where(((spot + 1) & (GROUP - 1)) != 0, spot + 1, -1)
            used_ref[0] = used + jnp.where(is_open, 0, 1)

    waiting = [(r, c) for r in range(ROWS) for c in range(chunks)]
    is_last_row = lax.broadcasted_iota(jnp.int32, (1, ROWS, LANES), 1) == ROWS - 1
    for c in range(chunks):
        cols = slice(c * LANES, (c + 1) * LANES)
        for k in range(0, levels, 5):
            here = slice(k, k + 5)
            flat = slice(k * ROWS, (k + 5) * ROWS)
            warm = t_ref[here, :, cols].astype(F32)
            rolled = pltpu.roll(warm, ROWS - 1, 1)
            carried = carry_ref[c, flat, :].reshape(5, ROWS, LANES)
            below = jnp.where(is_last_row, carried, rolled)
            carry_ref[c, flat, :] = rolled.reshape(5 * ROWS, LANES)
            flux = v_ref[here, :, cols].astype(F32) * (warm + below) * s_ref[here, :, cols]
            for q in range(5):
                at = (k + q) * PITCH
                flux_ref[c, at : at + ROWS, :] = flux[q]
            if waiting:
                enlist(*waiting.pop(0))
        for r in range(ROWS):
            cells = flux_ref[c, pl.ds(r, LEVEL_ROWS, stride=PITCH), :]
            runs_ref[(block * ROWS + r) * chunks + c] = cells.astype(BF16)

    bins = bin_ref[...]
    regs = reg_ref[...]
    code = bins - owner_of(bins, owned) * owned + (regs & 1) * LANES
    code = code.astype(F32)
    high = lax.shift_right_logical(regs, 1).astype(F32)
    for r in range(ROWS):
        for c in range(chunks):
            cols = slice(c * LANES, (c + 1) * LANES)
            run = (block * ROWS + r) * chunks + c
            tags_ref[run, 0] = jnp.broadcast_to(code[r : r + 1, cols], (16, LANES)).astype(BF16)
            tags_ref[run, 1] = jnp.broadcast_to(high[r : r + 1, cols], (16, LANES)).astype(BF16)

    @pl.when(step == 0)
    def _():
        edge_tags_ref[...] = tags_ref[spare - chunks : spare]

    @pl.when(step == last)
    def _():
        lists_ref[EDGE_AT + chunks] = used_ref[0]
        for c in range(chunks):
            row = carry_ref[c, pl.ds(ROWS - 1, LEVEL_ROWS, stride=ROWS), :]
            halo_ref[:, c * LANES : (c + 1) * LANES] = row.astype(BF16)


def stacked(x, n):
    return jnp.concatenate([x] * n, axis=0)


def group_sums(slot, tags_ref, members):
    lows, highs, spots = [], [], []
    one = jnp.ones((2 * LANES, LANES), BF16)
    nothing = jnp.zeros((2 * LANES, LANES), BF16)
    for cells, run in members:
        upper = cells * stacked(tags_ref[run, 1], LEVEL_ROWS // 16)
        lows.append(cells - upper)
        highs.append(upper)
        spots.append(jnp.where(slot == stacked(tags_ref[run, 0], 2 * LANES // 16), one, nothing))
    left = jnp.concatenate([jnp.concatenate(lows, axis=1), jnp.concatenate(highs, axis=1)], axis=0)
    right = jnp.concatenate(spots, axis=1)
    return lax.dot_general(left, right, (((1,), (1,)), ((), ())), preferred_element_type=F32)


def slots():
    return lax.broadcasted_iota(jnp.int32, (2 * LANES, LANES), 0).astype(F32).astype(BF16)


def sums_kernel(lists_ref, runs_ref, tags_ref, acc_ref):
    acc_ref[...] = jnp.zeros_like(acc_ref)
    slot = slots()
    chunks = lists_ref.shape[0] - EDGE_AT - 3

    def several(n, _):
        for u in range(UNROLL):
            group = n * UNROLL + u
            names = [lists_ref[GROUP * group + k] for k in range(GROUP)]
            own = lists_ref[OWNERS_AT + group]
            acc_ref[own] += group_sums(slot, tags_ref, [(runs_ref[a], a) for a in names])
        return 0

    used = lists_ref[EDGE_AT + chunks]
    lax.fori_loop(0, lax.div(used + UNROLL - 1, UNROLL), several, 0)


def edge_kernel(
    lists_ref, core_ref, halo_ref, tags_ref, edge_ref, sums_ref,
    acc_ref, keep_ref, send_ref,
):
    del sums_ref
    chunks = halo_ref.shape[1] // LANES
    owners = acc_ref.shape[0]
    slot = slots()
    for c in range(chunks):
        halo = halo_ref[:, c * LANES : (c + 1) * LANES].astype(F32)
        flux = (edge_ref[1, c] * (edge_ref[0, c] + halo) * edge_ref[2, c]).astype(BF16)
        acc_ref[lists_ref[EDGE_AT + c]] += group_sums(slot, tags_ref, [(flux, c)])
    core = core_ref[0]
    mine = pl.multiple_of(core * LEVEL_ROWS, LEVEL_ROWS)
    others = pl.multiple_of((1 - core) * LEVEL_ROWS, LEVEL_ROWS)
    for o in range(owners):
        keep_ref[o] = acc_ref[o, pl.ds(mine, LEVEL_ROWS), :]
        send_ref[o] = acc_ref[o, pl.ds(others, LEVEL_ROWS), :].astype(BF16)


def in_vmem(x):
    return pltpu.with_memory_space_constraint(x, pltpu.VMEM)


def in_hbm(x):
    return pltpu.with_memory_space_constraint(x, pltpu.HBM)


SMEM_WHOLE = pl.BlockSpec(memory_space=pltpu.SMEM)
VMEM_WHOLE = pl.BlockSpec(memory_space=pltpu.VMEM)


def local_runs(v, t, s, bins, regs, owned):
    levels, rows, cols = v.shape
    steps = rows // ROWS
    chunks = cols // LANES
    count = rows * chunks
    far = pl.BlockSpec(memory_space=pltpu.HBM)
    flat = pl.BlockSpec((ROWS, cols), lambda i: (steps - 1 - i, 0))
    flat_scalar = pl.BlockSpec((ROWS, cols), lambda i: (steps - 1 - i, 0), memory_space=pltpu.SMEM)

    def body(*refs):
        runs_kernel(owned, *refs)

    v, t, s, bins, regs = (in_hbm(x) for x in (v, t, s, bins, regs))
    return pl.pallas_call(
        body,
        grid=(steps,),
        in_specs=[far, far, far, flat, flat, flat_scalar],
        out_specs=[VMEM_WHOLE] * 5 + [SMEM_WHOLE],
        out_shape=[
            pltpu.VMEM((count + 1, LEVEL_ROWS, LANES), BF16),
            pltpu.VMEM((count + 1, 2, 16, LANES), BF16),
            pltpu.VMEM((3, chunks, LEVEL_ROWS, LANES), F32),
            pltpu.VMEM((chunks, 2, 16, LANES), BF16),
            pltpu.VMEM((LEVEL_ROWS, cols), BF16),
            jax.ShapeDtypeStruct((EDGE_AT + chunks + 3,), jnp.int32),
        ],
        scratch_shapes=[
            pltpu.VMEM((steps, levels, ROWS, cols), BF16),
            pltpu.VMEM((steps, levels, ROWS, cols), BF16),
            pltpu.VMEM((steps, levels, ROWS, cols), F32),
            pltpu.VMEM((chunks, LEVEL_ROWS * PITCH, LANES), F32),
            pltpu.VMEM((chunks, LEVEL_ROWS * ROWS, LANES), F32),
            pltpu.SMEM((17,), jnp.int32),
            pltpu.SMEM((1,), jnp.int32),
            pltpu.SemaphoreType.DMA((3, steps)),
        ],
        compiler_params=pltpu.CompilerParams(vmem_limit_bytes=32 * 1024 * 1024),
        name="runs", cost_estimate=pl.CostEstimate(flops=4000000000, bytes_accessed=20000000, transcendentals=0),
    )(v, t, s, bins, regs, bins)


def local_sums(lists, runs, tags):
    return pl.pallas_call(
        sums_kernel,
        in_specs=[SMEM_WHOLE, VMEM_WHOLE, VMEM_WHOLE],
        out_specs=VMEM_WHOLE,
        out_shape=pltpu.VMEM((16, 2 * LEVEL_ROWS, 2 * LANES), F32),
        compiler_params=pltpu.CompilerParams(vmem_limit_bytes=8 * 1024 * 1024),
        name="sums", cost_estimate=pl.CostEstimate(flops=4000000000, bytes_accessed=1000, transcendentals=0),
    )(lists, in_vmem(runs), in_vmem(tags))


def edge_sums(lists, core, halo, tags, edge, sums):
    owners = sums.shape[0]
    return pl.pallas_call(
        edge_kernel,
        in_specs=[SMEM_WHOLE, SMEM_WHOLE] + [VMEM_WHOLE] * 4,
        out_specs=[VMEM_WHOLE] * 3,
        out_shape=[
            pltpu.VMEM(sums.shape, F32),
            pltpu.VMEM((owners, LEVEL_ROWS, 2 * LANES), F32),
            pltpu.VMEM((owners, LEVEL_ROWS, 2 * LANES), BF16),
        ],
        input_output_aliases={5: 0},
        compiler_params=pltpu.CompilerParams(vmem_limit_bytes=8 * 1024 * 1024),
        name="edge",
    )(lists, core, in_vmem(halo), in_vmem(tags), in_vmem(edge), in_vmem(sums))[1:]


def assemble_kernel(scale, core_ref, mine_ref, other_ref, level_ref, total_ref):
    owners = mine_ref.shape[0]
    rows = level_ref.shape[1]
    owned = (BINS + owners - 1) // owners
    step = pl.program_id(0)
    first = core_ref[0] == 0
    lane = lax.broadcasted_iota(jnp.int32, (rows, LANES), 1)
    here = pl.ds(pl.multiple_of(step * rows, rows), rows)

    @pl.when(step == 0)
    def _():
        total_ref[...] = jnp.zeros_like(total_ref)

    def piece(o, q):
        side = slice((q % 2) * LANES, (q % 2 + 1) * LANES)
        a = mine_ref[o, here, side].astype(F32)
        b = other_ref[o, here, side].astype(F32)
        return jnp.where(first == (q < 2), a, b)

    tiles = (BINS + LANES - 1) // LANES
    for w in range(tiles):
        start = w * LANES
        width = min(LANES, BINS - start)
        regions = []
        for q in range(4):
            built = None
            for o in range(owners):
                lo = o * owned - start
                if lo >= width or lo + owned <= 0:
                    continue
                part = piece(o, q)
                if lo % LANES:
                    part = pltpu.roll(part, lo % LANES, 1)
                built = part if built is None else jnp.where(lane >= lo, part, built)
            regions.append(built)
        outs = [
            regions[0] + regions[1] + regions[2] + regions[3],
            regions[0],
            regions[1] + regions[2],
            regions[1],
            regions[2],
        ]
        for n in range(5):
            scaled = outs[n] * scale
            level_ref[n, :, start : start + width] = scaled[:, :width]
            total_ref[n : n + 1, start : start + width] += jnp.sum(
                scaled, axis=0, keepdims=True
            )[:, :width]


def assemble(core, mine, other, levels, scale):
    rows = 16
    vmem = pl.BlockSpec(memory_space=pltpu.VMEM)

    def body(*refs):
        assemble_kernel(scale, *refs)

    return pl.pallas_call(
        body,
        grid=(LEVEL_ROWS // rows,),
        in_specs=[pl.BlockSpec(memory_space=pltpu.SMEM), vmem, vmem],
        out_specs=[
            pl.BlockSpec((5, rows, BINS), lambda i: (0, i, 0)),
            pl.BlockSpec((5, BINS), lambda i: (0, 0)),
        ],
        out_shape=[
            jax.ShapeDtypeStruct((5, levels, BINS), F32),
            jax.ShapeDtypeStruct((5, BINS), F32),
        ],
        name="assemble",
    )(core, in_vmem(mine), in_vmem(other))


def shards(v, t, s, bins, regs):
    levels, rows, cols = v.shape
    owners = lax.axis_size("gy")
    count = lax.axis_size("gx")
    owned = (BINS + owners - 1) // owners
    check_owner_rule(owned)
    scale = 0.5 * (BINS / (rows * owners * cols * count)) ** 0.5
    core = lax.rem(lax.axis_index("gx"), 2).reshape(1)

    def swapped(x, bit):
        return lax.ppermute(x, "gx", [(k, k ^ bit) for k in range(count)])

    runs, tags, edge, edge_tags, first_row, lists = local_runs(v, t, s, bins, regs, owned)
    halo = lax.ppermute(first_row, "gy", [(k, k - 1) for k in range(1, owners)])
    sums = local_sums(lists, runs, tags)
    keep, send = edge_sums(lists, core, halo, edge_tags, edge, sums)
    paired = (keep + swapped(send, 1).astype(F32)).astype(BF16)
    arrived = lax.all_to_all(paired, "gy", 0, 0, tiled=True)
    own = arrived.astype(F32).sum(axis=0).astype(BF16)
    near, far, back = (
        lax.ppermute(own, "gx", [(k, (k + 2 * d) % count) for k in range(count)]).astype(F32)
        for d in (1, 2, 3)
    )
    whole = ((own.astype(F32) + far) + (near + back)).astype(BF16)
    spread = jnp.broadcast_to(whole[None], (owners, *whole.shape))
    mine = lax.all_to_all(spread, "gy", 0, 0, tiled=True)
    other = swapped(mine, 1)
    return tuple(assemble(core, mine, other, levels, scale))


def solution(mesh):
    return jax.shard_map(
        shards,
        mesh=mesh,
        in_specs=(
            P(None, "gy", "gx"),
            P(None, "gy", "gx"),
            P(None, "gy", "gx"),
            P("gy", "gx"),
            P("gy", "gx"),
        ),
        out_specs=(P(), P()),
        check_vma=False,
    )
```

```python
import jax
import jax.numpy as jnp
from jax import lax
from jax.experimental import pallas as pl
from jax.experimental.pallas import tpu as pltpu
from jax.sharding import PartitionSpec as P

BINS = 1800
ROWS = 8
PITCH = 9
AHEAD = 3
LANES = 128
LEVEL_ROWS = 80
GROUP = 4
GROUPS = 75
UNROLL = 5
EACH_STEP = 8
OWNERS_AT = GROUP * (GROUPS + 1)
TRASH_AT = OWNERS_AT + GROUPS + 1
READY_AT = TRASH_AT + 2
HEAD_AT = READY_AT + GROUPS + 16
COUNT_AT = HEAD_AT + 1
EDGE_AT = COUNT_AT + 1
BF16 = jnp.bfloat16
F32 = jnp.float32


def owner_of(bins, owned):
    factor = (1 << 16) // owned + 1
    return lax.shift_right_logical(bins * factor, 16)


def check_owner_rule(owned):
    factor = (1 << 16) // owned + 1
    assert all((b * factor) >> 16 == b // owned for b in range(BINS))


def runs_kernel(
    owned, v_hbm, t_hbm, s_hbm, bin_ref, reg_ref, first_ref,
    runs_ref, tags_ref, edge_ref, edge_tags_ref, halo_ref, acc_ref, lists_ref,
    v_all, t_all, s_all, flux_ref, carry_ref, open_ref, used_ref, sem_ref,
):
    steps, levels = v_all.shape[:2]
    chunks = v_all.shape[3] // LANES
    spare = runs_ref.shape[0] - 1
    step = pl.program_id(0)
    last = steps - 1
    block = last - step
    v_ref, t_ref, s_ref = v_all.at[step], t_all.at[step], s_all.at[step]

    def copies(i):
        rows = pl.ds(pl.multiple_of((last - i) * ROWS, ROWS), ROWS)
        return [
            pltpu.make_async_copy(far.at[:, rows, :], near.at[i], sem_ref.at[n, i])
            for n, (far, near) in enumerate(((t_hbm, t_all), (v_hbm, v_all), (s_hbm, s_all)))
        ]

    @pl.when(step == 0)
    def _():
        for i in range(AHEAD):
            for copy in copies(i):
                copy.start()

        carry_ref[...] = jnp.zeros_like(carry_ref)
        acc_ref[...] = jnp.zeros_like(acc_ref)
        lists_ref[HEAD_AT] = 0
        lists_ref[COUNT_AT] = 0
        flux_ref[...] = jnp.zeros_like(flux_ref)
        runs_ref[spare] = jnp.zeros((LEVEL_ROWS, LANES), BF16)
        tags_ref[spare, 0] = jnp.full((16, LANES), -1, BF16)
        tags_ref[spare, 1] = jnp.zeros((16, LANES), BF16)
        used_ref[0] = 0

        for n in range(OWNERS_AT):
            lists_ref[n] = spare
        for n in range(OWNERS_AT, TRASH_AT):
            lists_ref[n] = 0
        for o in range(17):
            open_ref[o] = -1

    for copy in copies(step):
        copy.wait()

    @pl.when(step < steps - AHEAD)
    def _():
        for copy in copies(step + AHEAD):
            copy.start()

    @pl.when(step == 0)
    def _():
        for c in range(chunks):
            cols = slice(c * LANES, (c + 1) * LANES)
            for n, ref in enumerate((t_ref, v_ref, s_ref)):
                for k in range(levels):
                    flux_ref[c, k * PITCH : k * PITCH + ROWS, :] = ref[k, :, cols].astype(F32)
                edge_ref[n, c] = flux_ref[c, pl.ds(ROWS - 1, LEVEL_ROWS, stride=PITCH), :]

    def enlist(r, c):
        live = True if r < ROWS - 1 else step > 0
        own = owner_of(first_ref[r, c * LANES], owned)
        if r == ROWS - 1:
            lists_ref[jnp.where(live, TRASH_AT + 1, EDGE_AT + c)] = own
        key = own if r < ROWS - 1 else jnp.where(live, own, 16)
        held = open_ref[key]
        used = used_ref[0]
        is_open = held >= 0
        spot = jnp.where(is_open, held, GROUP * used)
        if r == ROWS - 1:
            lists_ref[jnp.where(live, spot, TRASH_AT)] = (block * ROWS + r) * chunks + c
            lists_ref[jnp.where(live, OWNERS_AT + lax.shift_right_logical(spot, 2), TRASH_AT)] = own
            full = ((spot + 1) & (GROUP - 1)) == 0
            open_ref[key] = jnp.where(live & ~full, spot + 1, -1)
            used_ref[0] = used + jnp.where(live & ~is_open, 1, 0)
            full = full & live
        else:
            lists_ref[spot] = (block * ROWS + r) * chunks + c
            lists_ref[OWNERS_AT + lax.shift_right_logical(spot, 2)] = own
            full = ((spot + 1) & (GROUP - 1)) == 0
            open_ref[key] = jnp.where(full, -1, spot + 1)
            used_ref[0] = used + jnp.where(is_open, 0, 1)
        ready = lists_ref[COUNT_AT]
        lists_ref[READY_AT + ready] = lax.shift_right_logical(spot, 2)
        lists_ref[COUNT_AT] = ready + jnp.where(full, 1, 0)

    head = lists_ref[HEAD_AT]
    finished = lists_ref[COUNT_AT]
    lists_ref[HEAD_AT] = jnp.minimum(head + EACH_STEP, finished)
    chosen = [
        jnp.where(head + q < finished, lists_ref[READY_AT + head + q], GROUPS)
        for q in range(EACH_STEP)
    ]
    slot = slots()
    turn = 0

    waiting = [(r, c) for r in range(ROWS) for c in range(chunks)]
    is_last_row = lax.broadcasted_iota(jnp.int32, (1, ROWS, LANES), 1) == ROWS - 1
    for c in range(chunks):
        cols = slice(c * LANES, (c + 1) * LANES)
        for k in range(0, levels, 5):
            here = slice(k, k + 5)
            flat = slice(k * ROWS, (k + 5) * ROWS)
            warm = t_ref[here, :, cols].astype(F32)
            rolled = pltpu.roll(warm, ROWS - 1, 1)
            carried = carry_ref[c, flat, :].reshape(5, ROWS, LANES)
            below = jnp.where(is_last_row, carried, rolled)
            carry_ref[c, flat, :] = rolled.reshape(5 * ROWS, LANES)
            flux = v_ref[here, :, cols].astype(F32) * (warm + below) * s_ref[here, :, cols]
            for q in range(5):
                at = (k + q) * PITCH
                flux_ref[c, at : at + ROWS, :] = flux[q]
            if waiting:
                enlist(*waiting.pop(0))
            if turn % 5 == 2 and chosen:
                add_group(lists_ref, chosen.pop(0), slot, runs_ref, tags_ref, acc_ref)
            turn += 1
        for r in range(ROWS):
            cells = flux_ref[c, pl.ds(r, LEVEL_ROWS, stride=PITCH), :]
            runs_ref[(block * ROWS + r) * chunks + c] = cells.astype(BF16)

    bins = bin_ref[...]
    regs = reg_ref[...]
    code = bins - owner_of(bins, owned) * owned + (regs & 1) * LANES
    code = code.astype(F32)
    high = lax.shift_right_logical(regs, 1).astype(F32)
    for r in range(ROWS):
        for c in range(chunks):
            cols = slice(c * LANES, (c + 1) * LANES)
            run = (block * ROWS + r) * chunks + c
            tags_ref[run, 0] = jnp.broadcast_to(code[r : r + 1, cols], (16, LANES)).astype(BF16)
            tags_ref[run, 1] = jnp.broadcast_to(high[r : r + 1, cols], (16, LANES)).astype(BF16)

    @pl.when(step == 0)
    def _():
        edge_tags_ref[...] = tags_ref[spare - chunks : spare]

    @pl.when(step == last)
    def _():
        for o in range(16):
            held = open_ref[o]
            ready = lists_ref[COUNT_AT]
            lists_ref[READY_AT + ready] = lax.shift_right_logical(held, 2)
            lists_ref[COUNT_AT] = ready + jnp.where(held >= 0, 1, 0)
        ready = lists_ref[COUNT_AT]
        for n in range(UNROLL):
            lists_ref[READY_AT + ready + n] = GROUPS
        for c in range(chunks):
            row = carry_ref[c, pl.ds(ROWS - 1, LEVEL_ROWS, stride=ROWS), :]
            halo_ref[:, c * LANES : (c + 1) * LANES] = row.astype(BF16)


def stacked(x, n):
    return jnp.concatenate([x] * n, axis=0)


def group_sums(slot, tags_ref, members):
    lows, highs, spots = [], [], []
    one = jnp.ones((2 * LANES, LANES), BF16)
    nothing = jnp.zeros((2 * LANES, LANES), BF16)
    for cells, run in members:
        upper = cells * stacked(tags_ref[run, 1], LEVEL_ROWS // 16)
        lows.append(cells - upper)
        highs.append(upper)
        spots.append(jnp.where(slot == stacked(tags_ref[run, 0], 2 * LANES // 16), one, nothing))
    left = jnp.concatenate([jnp.concatenate(lows, axis=1), jnp.concatenate(highs, axis=1)], axis=0)
    right = jnp.concatenate(spots, axis=1)
    return lax.dot_general(left, right, (((1,), (1,)), ((), ())), preferred_element_type=F32)


def slots():
    return lax.broadcasted_iota(jnp.int32, (2 * LANES, LANES), 0).astype(F32).astype(BF16)


def add_group(lists_ref, group, slot, runs_ref, tags_ref, acc_ref):
    names = [lists_ref[GROUP * group + k] for k in range(GROUP)]
    own = lists_ref[OWNERS_AT + group]
    acc_ref[own] += group_sums(slot, tags_ref, [(runs_ref[a], a) for a in names])


def sums_kernel(lists_ref, runs_ref, tags_ref, first_ref, acc_ref):
    del first_ref
    slot = slots()
    head = lists_ref[HEAD_AT]
    count = lists_ref[COUNT_AT]

    def several(n, _):
        for u in range(UNROLL):
            group = lists_ref[READY_AT + head + n * UNROLL + u]
            add_group(lists_ref, group, slot, runs_ref, tags_ref, acc_ref)
        return 0

    lax.fori_loop(0, lax.div(count - head + UNROLL - 1, UNROLL), several, 0)


def edge_kernel(
    lists_ref, core_ref, halo_ref, tags_ref, edge_ref, sums_ref,
    acc_ref, keep_ref, send_ref,
):
    del sums_ref
    chunks = halo_ref.shape[1] // LANES
    owners = acc_ref.shape[0]
    slot = slots()
    for c in range(chunks):
        halo = halo_ref[:, c * LANES : (c + 1) * LANES].astype(F32)
        flux = (edge_ref[1, c] * (edge_ref[0, c] + halo) * edge_ref[2, c]).astype(BF16)
        acc_ref[lists_ref[EDGE_AT + c]] += group_sums(slot, tags_ref, [(flux, c)])
    core = core_ref[0]
    mine = pl.multiple_of(core * LEVEL_ROWS, LEVEL_ROWS)
    others = pl.multiple_of((1 - core) * LEVEL_ROWS, LEVEL_ROWS)
    for o in range(owners):
        keep_ref[o] = acc_ref[o, pl.ds(mine, LEVEL_ROWS), :]
        send_ref[o] = acc_ref[o, pl.ds(others, LEVEL_ROWS), :].astype(BF16)


def in_vmem(x):
    return pltpu.with_memory_space_constraint(x, pltpu.VMEM)


def in_hbm(x):
    return pltpu.with_memory_space_constraint(x, pltpu.HBM)


SMEM_WHOLE = pl.BlockSpec(memory_space=pltpu.SMEM)
VMEM_WHOLE = pl.BlockSpec(memory_space=pltpu.VMEM)


def local_runs(v, t, s, bins, regs, owned):
    levels, rows, cols = v.shape
    steps = rows // ROWS
    chunks = cols // LANES
    count = rows * chunks
    far = pl.BlockSpec(memory_space=pltpu.HBM)
    flat = pl.BlockSpec((ROWS, cols), lambda i: (steps - 1 - i, 0))
    flat_scalar = pl.BlockSpec((ROWS, cols), lambda i: (steps - 1 - i, 0), memory_space=pltpu.SMEM)

    def body(*refs):
        runs_kernel(owned, *refs)

    v, t, s, bins, regs = (in_hbm(x) for x in (v, t, s, bins, regs))
    return pl.pallas_call(
        body,
        grid=(steps,),
        in_specs=[far, far, far, flat, flat, flat_scalar],
        out_specs=[VMEM_WHOLE] * 6 + [SMEM_WHOLE],
        out_shape=[
            pltpu.VMEM((count + 1, LEVEL_ROWS, LANES), BF16),
            pltpu.VMEM((count + 1, 2, 16, LANES), BF16),
            pltpu.VMEM((3, chunks, LEVEL_ROWS, LANES), F32),
            pltpu.VMEM((chunks, 2, 16, LANES), BF16),
            pltpu.VMEM((LEVEL_ROWS, cols), BF16),
            pltpu.VMEM((16, 2 * LEVEL_ROWS, 2 * LANES), F32),
            jax.ShapeDtypeStruct((EDGE_AT + chunks,), jnp.int32),
        ],
        scratch_shapes=[
            pltpu.VMEM((steps, levels, ROWS, cols), BF16),
            pltpu.VMEM((steps, levels, ROWS, cols), BF16),
            pltpu.VMEM((steps, levels, ROWS, cols), F32),
            pltpu.VMEM((chunks, LEVEL_ROWS * PITCH, LANES), F32),
            pltpu.VMEM((chunks, LEVEL_ROWS * ROWS, LANES), F32),
            pltpu.SMEM((17,), jnp.int32),
            pltpu.SMEM((1,), jnp.int32),
            pltpu.SemaphoreType.DMA((3, steps)),
        ],
        compiler_params=pltpu.CompilerParams(vmem_limit_bytes=32 * 1024 * 1024),
        name="runs", cost_estimate=pl.CostEstimate(flops=4000000000, bytes_accessed=20000000, transcendentals=0),
    )(v, t, s, bins, regs, bins)


def local_sums(lists, runs, tags, begun):
    return pl.pallas_call(
        sums_kernel,
        in_specs=[SMEM_WHOLE, VMEM_WHOLE, VMEM_WHOLE, VMEM_WHOLE],
        out_specs=VMEM_WHOLE,
        input_output_aliases={3: 0},
        out_shape=pltpu.VMEM((16, 2 * LEVEL_ROWS, 2 * LANES), F32),
        compiler_params=pltpu.CompilerParams(vmem_limit_bytes=8 * 1024 * 1024),
        name="sums", cost_estimate=pl.CostEstimate(flops=4000000000, bytes_accessed=1000, transcendentals=0),
    )(lists, in_vmem(runs), in_vmem(tags), in_vmem(begun))


def edge_sums(lists, core, halo, tags, edge, sums):
    owners = sums.shape[0]
    return pl.pallas_call(
        edge_kernel,
        in_specs=[SMEM_WHOLE, SMEM_WHOLE] + [VMEM_WHOLE] * 4,
        out_specs=[VMEM_WHOLE] * 3,
        out_shape=[
            pltpu.VMEM(sums.shape, F32),
            pltpu.VMEM((owners, LEVEL_ROWS, 2 * LANES), F32),
            pltpu.VMEM((owners, LEVEL_ROWS, 2 * LANES), BF16),
        ],
        input_output_aliases={5: 0},
        compiler_params=pltpu.CompilerParams(vmem_limit_bytes=8 * 1024 * 1024),
        name="edge",
    )(lists, core, in_vmem(halo), in_vmem(tags), in_vmem(edge), in_vmem(sums))[1:]


def assemble_kernel(scale, core_ref, mine_ref, other_ref, level_ref, total_ref):
    owners = mine_ref.shape[0]
    rows = level_ref.shape[1]
    owned = (BINS + owners - 1) // owners
    step = pl.program_id(0)
    first = core_ref[0] == 0
    lane = lax.broadcasted_iota(jnp.int32, (rows, LANES), 1)
    here = pl.ds(pl.multiple_of(step * rows, rows), rows)

    @pl.when(step == 0)
    def _():
        total_ref[...] = jnp.zeros_like(total_ref)

    def piece(o, q):
        side = slice((q % 2) * LANES, (q % 2 + 1) * LANES)
        a = mine_ref[o, here, side].astype(F32)
        b = other_ref[o, here, side].astype(F32)
        return jnp.where(first == (q < 2), a, b)

    tiles = (BINS + LANES - 1) // LANES
    for w in range(tiles):
        start = w * LANES
        width = min(LANES, BINS - start)
        regions = []
        for q in range(4):
            built = None
            for o in range(owners):
                lo = o * owned - start
                if lo >= width or lo + owned <= 0:
                    continue
                part = piece(o, q)
                if lo % LANES:
                    part = pltpu.roll(part, lo % LANES, 1)
                built = part if built is None else jnp.where(lane >= lo, part, built)
            regions.append(built)
        outs = [
            regions[0] + regions[1] + regions[2] + regions[3],
            regions[0],
            regions[1] + regions[2],
            regions[1],
            regions[2],
        ]
        for n in range(5):
            scaled = outs[n] * scale
            level_ref[n, :, start : start + width] = scaled[:, :width]
            total_ref[n : n + 1, start : start + width] += jnp.sum(
                scaled, axis=0, keepdims=True
            )[:, :width]


def assemble(core, mine, other, levels, scale):
    rows = 16
    vmem = pl.BlockSpec(memory_space=pltpu.VMEM)

    def body(*refs):
        assemble_kernel(scale, *refs)

    return pl.pallas_call(
        body,
        grid=(LEVEL_ROWS // rows,),
        in_specs=[pl.BlockSpec(memory_space=pltpu.SMEM), vmem, vmem],
        out_specs=[
            pl.BlockSpec((5, rows, BINS), lambda i: (0, i, 0)),
            pl.BlockSpec((5, BINS), lambda i: (0, 0)),
        ],
        out_shape=[
            jax.ShapeDtypeStruct((5, levels, BINS), F32),
            jax.ShapeDtypeStruct((5, BINS), F32),
        ],
        name="assemble",
    )(core, in_vmem(mine), in_vmem(other))


def shards(v, t, s, bins, regs):
    levels, rows, cols = v.shape
    owners = lax.axis_size("gy")
    count = lax.axis_size("gx")
    owned = (BINS + owners - 1) // owners
    check_owner_rule(owned)
    scale = 0.5 * (BINS / (rows * owners * cols * count)) ** 0.5
    core = lax.rem(lax.axis_index("gx"), 2).reshape(1)

    def swapped(x, bit):
        return lax.ppermute(x, "gx", [(k, k ^ bit) for k in range(count)])

    runs, tags, edge, edge_tags, first_row, begun, lists = local_runs(v, t, s, bins, regs, owned)
    halo = lax.ppermute(first_row, "gy", [(k, k - 1) for k in range(1, owners)])
    sums = local_sums(lists, runs, tags, begun)
    keep, send = edge_sums(lists, core, halo, edge_tags, edge, sums)
    paired = (keep + swapped(send, 1).astype(F32)).astype(BF16)
    arrived = lax.all_to_all(paired, "gy", 0, 0, tiled=True)
    own = arrived.astype(F32).sum(axis=0).astype(BF16)
    near, far, back = (
        lax.ppermute(own, "gx", [(k, (k + 2 * d) % count) for k in range(count)]).astype(F32)
        for d in (1, 2, 3)
    )
    whole = ((own.astype(F32) + far) + (near + back)).astype(BF16)
    spread = jnp.broadcast_to(whole[None], (owners, *whole.shape))
    mine = lax.all_to_all(spread, "gy", 0, 0, tiled=True)
    other = swapped(mine, 1)
    return tuple(assemble(core, mine, other, levels, scale))


def solution(mesh):
    return jax.shard_map(
        shards,
        mesh=mesh,
        in_specs=(
            P(None, "gy", "gx"),
            P(None, "gy", "gx"),
            P(None, "gy", "gx"),
            P("gy", "gx"),
            P("gy", "gx"),
        ),
        out_specs=(P(), P()),
        check_vma=False,
    )
```

```python
import jax
import jax.numpy as jnp
from jax import lax
from jax.experimental import pallas as pl
from jax.experimental.pallas import tpu as pltpu
from jax.sharding import PartitionSpec as P

BINS = 1800
ROWS = 8
PITCH = 9
AHEAD = 3
LANES = 128
LEVEL_ROWS = 80
GROUP = 4
GROUPS = 75
UNROLL = 5
EACH_STEP = 8
OWNERS_AT = GROUP * (GROUPS + 1)
TRASH_AT = OWNERS_AT + GROUPS + 1
READY_AT = TRASH_AT + 2
HEAD_AT = READY_AT + GROUPS + 16
COUNT_AT = HEAD_AT + 1
EDGE_AT = COUNT_AT + 1
BF16 = jnp.bfloat16
F32 = jnp.float32


def owner_of(bins, owned):
    factor = (1 << 16) // owned + 1
    return lax.shift_right_logical(bins * factor, 16)


def check_owner_rule(owned):
    factor = (1 << 16) // owned + 1
    assert all((b * factor) >> 16 == b // owned for b in range(BINS))


def runs_kernel(
    owned, v_hbm, t_hbm, s_hbm, bin_ref, reg_ref, first_ref,
    runs_ref, tags_ref, edge_ref, edge_tags_ref, acc_ref, lists_ref,
    v_all, t_all, s_all, flux_ref, carry_ref, open_ref, used_ref, sem_ref,
):
    steps, levels = v_all.shape[:2]
    chunks = v_all.shape[3] // LANES
    spare = runs_ref.shape[0] - 1
    step = pl.program_id(0)
    last = steps - 1
    block = last - step
    v_ref, t_ref, s_ref = v_all.at[step], t_all.at[step], s_all.at[step]

    def copies(i):
        rows = pl.ds(pl.multiple_of((last - i) * ROWS, ROWS), ROWS)
        return [
            pltpu.make_async_copy(far.at[:, rows, :], near.at[i], sem_ref.at[n, i])
            for n, (far, near) in enumerate(((t_hbm, t_all), (v_hbm, v_all), (s_hbm, s_all)))
        ]

    @pl.when(step == 0)
    def _():
        for i in range(AHEAD):
            for copy in copies(i):
                copy.start()

        carry_ref[...] = jnp.zeros_like(carry_ref)
        acc_ref[...] = jnp.zeros_like(acc_ref)
        lists_ref[HEAD_AT] = 0
        lists_ref[COUNT_AT] = 0
        flux_ref[...] = jnp.zeros_like(flux_ref)
        runs_ref[spare] = jnp.zeros((LEVEL_ROWS, LANES), BF16)
        tags_ref[spare, 0] = jnp.full((16, LANES), -1, BF16)
        tags_ref[spare, 1] = jnp.zeros((16, LANES), BF16)
        used_ref[0] = 0

        for n in range(OWNERS_AT):
            lists_ref[n] = spare
        for n in range(OWNERS_AT, TRASH_AT):
            lists_ref[n] = 0
        for o in range(17):
            open_ref[o] = -1

    for copy in copies(step):
        copy.wait()

    @pl.when(step < steps - AHEAD)
    def _():
        for copy in copies(step + AHEAD):
            copy.start()

    @pl.when(step == 0)
    def _():
        for c in range(chunks):
            cols = slice(c * LANES, (c + 1) * LANES)
            for n, ref in enumerate((t_ref, v_ref, s_ref)):
                for k in range(levels):
                    flux_ref[c, k * PITCH : k * PITCH + ROWS, :] = ref[k, :, cols].astype(F32)
                edge_ref[n, c] = flux_ref[c, pl.ds(ROWS - 1, LEVEL_ROWS, stride=PITCH), :]

    def enlist(r, c):
        live = True if r < ROWS - 1 else step > 0
        own = owner_of(first_ref[r, c * LANES], owned)
        if r == ROWS - 1:
            lists_ref[jnp.where(live, TRASH_AT + 1, EDGE_AT + c)] = own
        key = own if r < ROWS - 1 else jnp.where(live, own, 16)
        held = open_ref[key]
        used = used_ref[0]
        is_open = held >= 0
        spot = jnp.where(is_open, held, GROUP * used)
        if r == ROWS - 1:
            lists_ref[jnp.where(live, spot, TRASH_AT)] = (block * ROWS + r) * chunks + c
            lists_ref[jnp.where(live, OWNERS_AT + lax.shift_right_logical(spot, 2), TRASH_AT)] = own
            full = ((spot + 1) & (GROUP - 1)) == 0
            open_ref[key] = jnp.where(live & ~full, spot + 1, -1)
            used_ref[0] = used + jnp.where(live & ~is_open, 1, 0)
            full = full & live
        else:
            lists_ref[spot] = (block * ROWS + r) * chunks + c
            lists_ref[OWNERS_AT + lax.shift_right_logical(spot, 2)] = own
            full = ((spot + 1) & (GROUP - 1)) == 0
            open_ref[key] = jnp.where(full, -1, spot + 1)
            used_ref[0] = used + jnp.where(is_open, 0, 1)
        ready = lists_ref[COUNT_AT]
        lists_ref[READY_AT + ready] = lax.shift_right_logical(spot, 2)
        lists_ref[COUNT_AT] = ready + jnp.where(full, 1, 0)

    head = lists_ref[HEAD_AT]
    finished = lists_ref[COUNT_AT]
    lists_ref[HEAD_AT] = jnp.minimum(head + EACH_STEP, finished)
    chosen = [
        jnp.where(head + q < finished, lists_ref[READY_AT + head + q], GROUPS)
        for q in range(EACH_STEP)
    ]
    slot = slots()
    turn = 0

    waiting = [(r, c) for r in range(ROWS) for c in range(chunks)]
    is_last_row = lax.broadcasted_iota(jnp.int32, (1, ROWS, LANES), 1) == ROWS - 1
    for c in range(chunks):
        cols = slice(c * LANES, (c + 1) * LANES)
        for k in range(0, levels, 5):
            here = slice(k, k + 5)
            flat = slice(k * ROWS, (k + 5) * ROWS)
            warm = t_ref[here, :, cols].astype(F32)
            rolled = pltpu.roll(warm, ROWS - 1, 1)
            carried = carry_ref[c, flat, :].reshape(5, ROWS, LANES)
            below = jnp.where(is_last_row, carried, rolled)
            carry_ref[c, flat, :] = rolled.reshape(5 * ROWS, LANES)
            flux = v_ref[here, :, cols].astype(F32) * (warm + below) * s_ref[here, :, cols]
            for q in range(5):
                at = (k + q) * PITCH
                flux_ref[c, at : at + ROWS, :] = flux[q]
            if waiting:
                enlist(*waiting.pop(0))
            if turn % 5 == 2 and chosen:
                add_group(lists_ref, chosen.pop(0), slot, runs_ref, tags_ref, acc_ref)
            turn += 1
        for r in range(ROWS):
            cells = flux_ref[c, pl.ds(r, LEVEL_ROWS, stride=PITCH), :]
            runs_ref[(block * ROWS + r) * chunks + c] = cells.astype(BF16)

    bins = bin_ref[...]
    regs = reg_ref[...]
    code = bins - owner_of(bins, owned) * owned + (regs & 1) * LANES
    code = code.astype(F32)
    high = lax.shift_right_logical(regs, 1).astype(F32)
    for r in range(ROWS):
        for c in range(chunks):
            cols = slice(c * LANES, (c + 1) * LANES)
            run = (block * ROWS + r) * chunks + c
            tags_ref[run, 0] = jnp.broadcast_to(code[r : r + 1, cols], (16, LANES)).astype(BF16)
            tags_ref[run, 1] = jnp.broadcast_to(high[r : r + 1, cols], (16, LANES)).astype(BF16)

    @pl.when(step == 0)
    def _():
        edge_tags_ref[...] = tags_ref[spare - chunks : spare]

    @pl.when(step == last)
    def _():
        for o in range(16):
            held = open_ref[o]
            ready = lists_ref[COUNT_AT]
            lists_ref[READY_AT + ready] = lax.shift_right_logical(held, 2)
            lists_ref[COUNT_AT] = ready + jnp.where(held >= 0, 1, 0)
        ready = lists_ref[COUNT_AT]
        for n in range(UNROLL):
            lists_ref[READY_AT + ready + n] = GROUPS


def stacked(x, n):
    return jnp.concatenate([x] * n, axis=0)


def group_sums(slot, tags_ref, members):
    lows, highs, spots = [], [], []
    one = jnp.ones((2 * LANES, LANES), BF16)
    nothing = jnp.zeros((2 * LANES, LANES), BF16)
    for cells, run in members:
        upper = cells * stacked(tags_ref[run, 1], LEVEL_ROWS // 16)
        lows.append(cells - upper)
        highs.append(upper)
        spots.append(jnp.where(slot == stacked(tags_ref[run, 0], 2 * LANES // 16), one, nothing))
    left = jnp.concatenate([jnp.concatenate(lows, axis=1), jnp.concatenate(highs, axis=1)], axis=0)
    right = jnp.concatenate(spots, axis=1)
    return lax.dot_general(left, right, (((1,), (1,)), ((), ())), preferred_element_type=F32)


def slots():
    return lax.broadcasted_iota(jnp.int32, (2 * LANES, LANES), 0).astype(F32).astype(BF16)


def add_group(lists_ref, group, slot, runs_ref, tags_ref, acc_ref):
    names = [lists_ref[GROUP * group + k] for k in range(GROUP)]
    own = lists_ref[OWNERS_AT + group]
    acc_ref[own] += group_sums(slot, tags_ref, [(runs_ref[a], a) for a in names])


def sums_kernel(
    lists_ref, place_ref, halo_ref, runs_ref, tags_ref, edge_ref, edge_tags_ref, begun_ref,
    acc_ref, keep_ref, send_ref, halo32_ref,
):
    del begun_ref
    levels, cols = halo_ref.shape
    owners = acc_ref.shape[0]
    slot = slots()
    head = lists_ref[HEAD_AT]
    count = lists_ref[COUNT_AT]
    halo = jnp.where(place_ref[1] == 0, halo_ref[...].astype(F32), 0.0)
    halo32_ref[:levels] = halo
    halo32_ref[levels:] = jnp.zeros((LEVEL_ROWS - levels, cols), F32)

    def several(n, _):
        for u in range(UNROLL):
            group = lists_ref[READY_AT + head + n * UNROLL + u]
            add_group(lists_ref, group, slot, runs_ref, tags_ref, acc_ref)
        return 0

    lax.fori_loop(0, lax.div(count - head + UNROLL - 1, UNROLL), several, 0)

    for c in range(cols // LANES):
        warm = edge_ref[0, c] + halo32_ref[:, c * LANES : (c + 1) * LANES]
        flux = (edge_ref[1, c] * warm * edge_ref[2, c]).astype(BF16)
        acc_ref[lists_ref[EDGE_AT + c]] += group_sums(slot, edge_tags_ref, [(flux, c)])
    core = place_ref[0]
    mine = pl.multiple_of(core * LEVEL_ROWS, LEVEL_ROWS)
    others = pl.multiple_of((1 - core) * LEVEL_ROWS, LEVEL_ROWS)
    for o in range(owners):
        keep_ref[o] = acc_ref[o, pl.ds(mine, LEVEL_ROWS), :]
        send_ref[o] = acc_ref[o, pl.ds(others, LEVEL_ROWS), :].astype(BF16)


def in_vmem(x):
    return pltpu.with_memory_space_constraint(x, pltpu.VMEM)


def in_hbm(x):
    return pltpu.with_memory_space_constraint(x, pltpu.HBM)


SMEM_WHOLE = pl.BlockSpec(memory_space=pltpu.SMEM)
VMEM_WHOLE = pl.BlockSpec(memory_space=pltpu.VMEM)


def local_runs(v, t, s, bins, regs, owned):
    levels, rows, cols = v.shape
    steps = rows // ROWS
    chunks = cols // LANES
    count = rows * chunks
    far = pl.BlockSpec(memory_space=pltpu.HBM)
    flat = pl.BlockSpec((ROWS, cols), lambda i: (steps - 1 - i, 0))
    flat_scalar = pl.BlockSpec((ROWS, cols), lambda i: (steps - 1 - i, 0), memory_space=pltpu.SMEM)

    def body(*refs):
        runs_kernel(owned, *refs)

    v, t, s, bins, regs = (in_hbm(x) for x in (v, t, s, bins, regs))
    return pl.pallas_call(
        body,
        grid=(steps,),
        in_specs=[far, far, far, flat, flat, flat_scalar],
        out_specs=[VMEM_WHOLE] * 5 + [SMEM_WHOLE],
        out_shape=[
            pltpu.VMEM((count + 1, LEVEL_ROWS, LANES), BF16),
            pltpu.VMEM((count + 1, 2, 16, LANES), BF16),
            pltpu.VMEM((3, chunks, LEVEL_ROWS, LANES), F32),
            pltpu.VMEM((chunks, 2, 16, LANES), BF16),
            pltpu.VMEM((16, 2 * LEVEL_ROWS, 2 * LANES), F32),
            jax.ShapeDtypeStruct((EDGE_AT + chunks,), jnp.int32),
        ],
        scratch_shapes=[
            pltpu.VMEM((steps, levels, ROWS, cols), BF16),
            pltpu.VMEM((steps, levels, ROWS, cols), BF16),
            pltpu.VMEM((steps, levels, ROWS, cols), F32),
            pltpu.VMEM((chunks, LEVEL_ROWS * PITCH, LANES), F32),
            pltpu.VMEM((chunks, LEVEL_ROWS * ROWS, LANES), F32),
            pltpu.SMEM((17,), jnp.int32),
            pltpu.SMEM((1,), jnp.int32),
            pltpu.SemaphoreType.DMA((3, steps)),
        ],
        compiler_params=pltpu.CompilerParams(vmem_limit_bytes=32 * 1024 * 1024),
        name="runs", cost_estimate=pl.CostEstimate(flops=4000000000, bytes_accessed=20000000, transcendentals=0),
    )(v, t, s, bins, regs, bins)


def local_sums(lists, place, halo, runs, tags, edge, edge_tags, begun):
    owners = begun.shape[0]
    values = [in_vmem(x) for x in (halo, runs, tags, edge, edge_tags, begun)]
    return pl.pallas_call(
        sums_kernel,
        in_specs=[SMEM_WHOLE, SMEM_WHOLE] + [VMEM_WHOLE] * 6,
        out_specs=[VMEM_WHOLE] * 3,
        out_shape=[
            pltpu.VMEM(begun.shape, F32),
            pltpu.VMEM((owners, LEVEL_ROWS, 2 * LANES), F32),
            pltpu.VMEM((owners, LEVEL_ROWS, 2 * LANES), BF16),
        ],
        input_output_aliases={7: 0},
        scratch_shapes=[pltpu.VMEM((LEVEL_ROWS, halo.shape[1]), F32)],
        compiler_params=pltpu.CompilerParams(vmem_limit_bytes=8 * 1024 * 1024),
        name="sums", cost_estimate=pl.CostEstimate(flops=4000000000, bytes_accessed=1000, transcendentals=0),
    )(lists, place, *values)[1:]


def assemble_kernel(scale, core_ref, mine_ref, other_ref, level_ref, total_ref):
    owners = mine_ref.shape[0]
    rows = level_ref.shape[1]
    owned = (BINS + owners - 1) // owners
    step = pl.program_id(0)
    first = core_ref[0] == 0
    lane = lax.broadcasted_iota(jnp.int32, (rows, LANES), 1)
    here = pl.ds(pl.multiple_of(step * rows, rows), rows)

    @pl.when(step == 0)
    def _():
        total_ref[...] = jnp.zeros_like(total_ref)

    def piece(o, q):
        side = slice((q % 2) * LANES, (q % 2 + 1) * LANES)
        a = mine_ref[o, here, side].astype(F32)
        b = other_ref[o, here, side].astype(F32)
        return jnp.where(first == (q < 2), a, b)

    tiles = (BINS + LANES - 1) // LANES
    for w in range(tiles):
        start = w * LANES
        width = min(LANES, BINS - start)
        regions = []
        for q in range(4):
            built = None
            for o in range(owners):
                lo = o * owned - start
                if lo >= width or lo + owned <= 0:
                    continue
                part = piece(o, q)
                if lo % LANES:
                    part = pltpu.roll(part, lo % LANES, 1)
                built = part if built is None else jnp.where(lane >= lo, part, built)
            regions.append(built)
        outs = [
            regions[0] + regions[1] + regions[2] + regions[3],
            regions[0],
            regions[1] + regions[2],
            regions[1],
            regions[2],
        ]
        for n in range(5):
            scaled = outs[n] * scale
            level_ref[n, :, start : start + width] = scaled[:, :width]
            total_ref[n : n + 1, start : start + width] += jnp.sum(
                scaled, axis=0, keepdims=True
            )[:, :width]


def assemble(core, mine, other, levels, scale):
    rows = 16
    vmem = pl.BlockSpec(memory_space=pltpu.VMEM)

    def body(*refs):
        assemble_kernel(scale, *refs)

    return pl.pallas_call(
        body,
        grid=(LEVEL_ROWS // rows,),
        in_specs=[pl.BlockSpec(memory_space=pltpu.SMEM), vmem, vmem],
        out_specs=[
            pl.BlockSpec((5, rows, BINS), lambda i: (0, i, 0)),
            pl.BlockSpec((5, BINS), lambda i: (0, 0)),
        ],
        out_shape=[
            jax.ShapeDtypeStruct((5, levels, BINS), F32),
            jax.ShapeDtypeStruct((5, BINS), F32),
        ],
        name="assemble",
    )(core, in_vmem(mine), in_vmem(other))


def shards(v, t, s, bins, regs):
    levels, rows, cols = v.shape
    owners = lax.axis_size("gy")
    count = lax.axis_size("gx")
    owned = (BINS + owners - 1) // owners
    check_owner_rule(owned)
    scale = 0.5 * (BINS / (rows * owners * cols * count)) ** 0.5
    core = lax.rem(lax.axis_index("gx"), 2).reshape(1)

    def swapped(x, bit):
        return lax.ppermute(x, "gx", [(k, k ^ bit) for k in range(count)])

    is_last = (lax.axis_index("gy") == owners - 1).astype(jnp.int32)
    place = jnp.concatenate([core, is_last.reshape(1)])
    halo = lax.ppermute(t[:, 0, :], "gy", [(k, (k - 1) % owners) for k in range(owners)])
    runs, tags, edge, edge_tags, begun, lists = local_runs(v, t, s, bins, regs, owned)
    keep, send = local_sums(lists, place, halo, runs, tags, edge, edge_tags, begun)
    paired = (keep + swapped(send, 1).astype(F32)).astype(BF16)
    arrived = lax.all_to_all(paired, "gy", 0, 0, tiled=True)
    own = arrived.astype(F32).sum(axis=0).astype(BF16)
    near, far, back = (
        lax.ppermute(own, "gx", [(k, (k + 2 * d) % count) for k in range(count)]).astype(F32)
        for d in (1, 2, 3)
    )
    whole = ((own.astype(F32) + far) + (near + back)).astype(BF16)
    spread = jnp.broadcast_to(whole[None], (owners, *whole.shape))
    mine = lax.all_to_all(spread, "gy", 0, 0, tiled=True)
    other = swapped(mine, 1)
    return tuple(assemble(core, mine, other, levels, scale))


def solution(mesh):
    return jax.shard_map(
        shards,
        mesh=mesh,
        in_specs=(
            P(None, "gy", "gx"),
            P(None, "gy", "gx"),
            P(None, "gy", "gx"),
            P("gy", "gx"),
            P("gy", "gx"),
        ),
        out_specs=(P(), P()),
        check_vma=False,
    )
```

```python
import jax
import jax.numpy as jnp
from jax import lax
from jax.experimental import pallas as pl
from jax.experimental.pallas import tpu as pltpu
from jax.sharding import PartitionSpec as P

BINS = 1800
ROWS = 8
PITCH = 9
AHEAD = 3
LANES = 128
LEVEL_ROWS = 80
GROUP = 4
GROUPS = 75
UNROLL = 5
EACH_STEP = 8
OWNERS_AT = GROUP * (GROUPS + 1)
TRASH_AT = OWNERS_AT + GROUPS + 1
READY_AT = TRASH_AT + 2
HEAD_AT = READY_AT + GROUPS + 16
COUNT_AT = HEAD_AT + 1
EDGE_AT = COUNT_AT + 1
BF16 = jnp.bfloat16
F32 = jnp.float32


def owner_of(bins, owned):
    factor = (1 << 16) // owned + 1
    return lax.shift_right_logical(bins * factor, 16)


def check_owner_rule(owned):
    factor = (1 << 16) // owned + 1
    assert all((b * factor) >> 16 == b // owned for b in range(BINS))


def runs_kernel(
    owned, v_hbm, t_hbm, s_hbm, bin_ref, reg_ref, first_ref,
    runs_ref, tags_ref, edge_ref, edge_tags_ref, acc_ref, lists_ref,
    v_all, t_all, s_all, flux_ref, carry_ref, open_ref, used_ref, sem_ref,
):
    steps, levels = v_all.shape[:2]
    chunks = v_all.shape[3] // LANES
    spare = runs_ref.shape[0] - 1
    step = pl.program_id(0)
    last = steps - 1
    block = last - step
    v_ref, t_ref, s_ref = v_all.at[step], t_all.at[step], s_all.at[step]

    def copies(i):
        rows = pl.ds(pl.multiple_of((last - i) * ROWS, ROWS), ROWS)
        return [
            pltpu.make_async_copy(far.at[:, rows, :], near.at[i], sem_ref.at[n, i])
            for n, (far, near) in enumerate(((t_hbm, t_all), (v_hbm, v_all), (s_hbm, s_all)))
        ]

    @pl.when(step == 0)
    def _():
        for i in range(AHEAD):
            for copy in copies(i):
                copy.start()

        carry_ref[...] = jnp.zeros_like(carry_ref)
        acc_ref[...] = jnp.zeros_like(acc_ref)
        lists_ref[HEAD_AT] = 0
        lists_ref[COUNT_AT] = 0
        flux_ref[...] = jnp.zeros_like(flux_ref)
        runs_ref[spare] = jnp.zeros((LEVEL_ROWS, LANES), BF16)
        tags_ref[spare, 0] = jnp.full((16, LANES), -1, BF16)
        tags_ref[spare, 1] = jnp.zeros((16, LANES), BF16)
        used_ref[0] = 0

        for n in range(OWNERS_AT):
            lists_ref[n] = spare
        for n in range(OWNERS_AT, TRASH_AT):
            lists_ref[n] = 0
        for o in range(17):
            open_ref[o] = -1

    for copy in copies(step):
        copy.wait()

    @pl.when(step < steps - AHEAD)
    def _():
        for copy in copies(step + AHEAD):
            copy.start()

    @pl.when(step == 0)
    def _():
        for c in range(chunks):
            cols = slice(c * LANES, (c + 1) * LANES)
            for n, ref in enumerate((t_ref, v_ref, s_ref)):
                for k in range(levels):
                    flux_ref[c, k * PITCH : k * PITCH + ROWS, :] = ref[k, :, cols].astype(F32)
                edge_ref[n, c] = flux_ref[c, pl.ds(ROWS - 1, LEVEL_ROWS, stride=PITCH), :]

    def enlist(r, c):
        live = True if r < ROWS - 1 else step > 0
        own = owner_of(first_ref[r, c * LANES], owned)
        if r == ROWS - 1:
            lists_ref[jnp.where(live, TRASH_AT + 1, EDGE_AT + c)] = own
        key = own if r < ROWS - 1 else jnp.where(live, own, 16)
        held = open_ref[key]
        used = used_ref[0]
        is_open = held >= 0
        spot = jnp.where(is_open, held, GROUP * used)
        if r == ROWS - 1:
            lists_ref[jnp.where(live, spot, TRASH_AT)] = (block * ROWS + r) * chunks + c
            lists_ref[jnp.where(live, OWNERS_AT + lax.shift_right_logical(spot, 2), TRASH_AT)] = own
            full = ((spot + 1) & (GROUP - 1)) == 0
            open_ref[key] = jnp.where(live & ~full, spot + 1, -1)
            used_ref[0] = used + jnp.where(live & ~is_open, 1, 0)
            full = full & live
        else:
            lists_ref[spot] = (block * ROWS + r) * chunks + c
            lists_ref[OWNERS_AT + lax.shift_right_logical(spot, 2)] = own
            full = ((spot + 1) & (GROUP - 1)) == 0
            open_ref[key] = jnp.where(full, -1, spot + 1)
            used_ref[0] = used + jnp.where(is_open, 0, 1)
        ready = lists_ref[COUNT_AT]
        lists_ref[READY_AT + ready] = lax.shift_right_logical(spot, 2)
        lists_ref[COUNT_AT] = ready + jnp.where(full, 1, 0)

    def main_part(each):
        head = lists_ref[HEAD_AT]
        finished = lists_ref[COUNT_AT]
        lists_ref[HEAD_AT] = jnp.minimum(head + each, finished)
        chosen = [
            jnp.where(head + q < finished, lists_ref[READY_AT + head + q], GROUPS)
            for q in range(each)
        ]
        slot = slots()
        turn = 0

        waiting = [(r, c) for r in range(ROWS) for c in range(chunks)]
        is_last_row = lax.broadcasted_iota(jnp.int32, (1, ROWS, LANES), 1) == ROWS - 1
        for c in range(chunks):
            cols = slice(c * LANES, (c + 1) * LANES)
            for k in range(0, levels, 5):
                here = slice(k, k + 5)
                flat = slice(k * ROWS, (k + 5) * ROWS)
                warm = t_ref[here, :, cols].astype(F32)
                rolled = pltpu.roll(warm, ROWS - 1, 1)
                carried = carry_ref[c, flat, :].reshape(5, ROWS, LANES)
                below = jnp.where(is_last_row, carried, rolled)
                carry_ref[c, flat, :] = rolled.reshape(5 * ROWS, LANES)
                flux = v_ref[here, :, cols].astype(F32) * (warm + below) * s_ref[here, :, cols]
                for q in range(5):
                    at = (k + q) * PITCH
                    flux_ref[c, at : at + ROWS, :] = flux[q]
                if waiting:
                    enlist(*waiting.pop(0))
                if turn % 5 == 2 and chosen:
                    add_group(lists_ref, chosen.pop(0), slot, runs_ref, tags_ref, acc_ref)
                turn += 1
            for r in range(ROWS):
                cells = flux_ref[c, pl.ds(r, LEVEL_ROWS, stride=PITCH), :]
                runs_ref[(block * ROWS + r) * chunks + c] = cells.astype(BF16)

    @pl.when(step == 0)
    def _():
        main_part(0)

    @pl.when(step > 0)
    def _():
        main_part(EACH_STEP)

    bins = bin_ref[...]
    regs = reg_ref[...]
    code = bins - owner_of(bins, owned) * owned + (regs & 1) * LANES
    code = code.astype(F32)
    high = lax.shift_right_logical(regs, 1).astype(F32)
    for r in range(ROWS):
        for c in range(chunks):
            cols = slice(c * LANES, (c + 1) * LANES)
            run = (block * ROWS + r) * chunks + c
            tags_ref[run, 0] = jnp.broadcast_to(code[r : r + 1, cols], (16, LANES)).astype(BF16)
            tags_ref[run, 1] = jnp.broadcast_to(high[r : r + 1, cols], (16, LANES)).astype(BF16)

    @pl.when(step == 0)
    def _():
        edge_tags_ref[...] = tags_ref[spare - chunks : spare]

    @pl.when(step == last)
    def _():
        for o in range(16):
            held = open_ref[o]
            ready = lists_ref[COUNT_AT]
            lists_ref[READY_AT + ready] = lax.shift_right_logical(held, 2)
            lists_ref[COUNT_AT] = ready + jnp.where(held >= 0, 1, 0)
        ready = lists_ref[COUNT_AT]
        for n in range(UNROLL):
            lists_ref[READY_AT + ready + n] = GROUPS


def stacked(x, n):
    return jnp.concatenate([x] * n, axis=0)


def group_sums(slot, tags_ref, members):
    lows, highs, spots = [], [], []
    one = jnp.ones((2 * LANES, LANES), BF16)
    nothing = jnp.zeros((2 * LANES, LANES), BF16)
    for cells, run in members:
        upper = cells * stacked(tags_ref[run, 1], LEVEL_ROWS // 16)
        lows.append(cells - upper)
        highs.append(upper)
        spots.append(jnp.where(slot == stacked(tags_ref[run, 0], 2 * LANES // 16), one, nothing))
    left = jnp.concatenate([jnp.concatenate(lows, axis=1), jnp.concatenate(highs, axis=1)], axis=0)
    right = jnp.concatenate(spots, axis=1)
    return lax.dot_general(left, right, (((1,), (1,)), ((), ())), preferred_element_type=F32)


def slots():
    return lax.broadcasted_iota(jnp.int32, (2 * LANES, LANES), 0).astype(F32).astype(BF16)


def add_group(lists_ref, group, slot, runs_ref, tags_ref, acc_ref):
    names = [lists_ref[GROUP * group + k] for k in range(GROUP)]
    own = lists_ref[OWNERS_AT + group]
    acc_ref[own] += group_sums(slot, tags_ref, [(runs_ref[a], a) for a in names])


def sums_kernel(
    lists_ref, place_ref, halo_ref, runs_ref, tags_ref, edge_ref, edge_tags_ref, begun_ref,
    acc_ref, keep_ref, send_ref, halo32_ref,
):
    del begun_ref
    levels, cols = halo_ref.shape
    owners = acc_ref.shape[0]
    slot = slots()
    head = lists_ref[HEAD_AT]
    count = lists_ref[COUNT_AT]
    halo = jnp.where(place_ref[1] == 0, halo_ref[...].astype(F32), 0.0)
    halo32_ref[:levels] = halo
    halo32_ref[levels:] = jnp.zeros((LEVEL_ROWS - levels, cols), F32)

    def several(n, _):
        for u in range(UNROLL):
            group = lists_ref[READY_AT + head + n * UNROLL + u]
            add_group(lists_ref, group, slot, runs_ref, tags_ref, acc_ref)
        return 0

    lax.fori_loop(0, lax.div(count - head + UNROLL - 1, UNROLL), several, 0)

    for c in range(cols // LANES):
        warm = edge_ref[0, c] + halo32_ref[:, c * LANES : (c + 1) * LANES]
        flux = (edge_ref[1, c] * warm * edge_ref[2, c]).astype(BF16)
        acc_ref[lists_ref[EDGE_AT + c]] += group_sums(slot, edge_tags_ref, [(flux, c)])
    core = place_ref[0]
    mine = pl.multiple_of(core * LEVEL_ROWS, LEVEL_ROWS)
    others = pl.multiple_of((1 - core) * LEVEL_ROWS, LEVEL_ROWS)
    for o in range(owners):
        keep_ref[o] = acc_ref[o, pl.ds(mine, LEVEL_ROWS), :]
        send_ref[o] = acc_ref[o, pl.ds(others, LEVEL_ROWS), :].astype(BF16)


def in_vmem(x):
    return pltpu.with_memory_space_constraint(x, pltpu.VMEM)


def in_hbm(x):
    return pltpu.with_memory_space_constraint(x, pltpu.HBM)


SMEM_WHOLE = pl.BlockSpec(memory_space=pltpu.SMEM)
VMEM_WHOLE = pl.BlockSpec(memory_space=pltpu.VMEM)


def local_runs(v, t, s, bins, regs, owned):
    levels, rows, cols = v.shape
    steps = rows // ROWS
    chunks = cols // LANES
    count = rows * chunks
    far = pl.BlockSpec(memory_space=pltpu.HBM)
    flat = pl.BlockSpec((ROWS, cols), lambda i: (steps - 1 - i, 0))
    flat_scalar = pl.BlockSpec((ROWS, cols), lambda i: (steps - 1 - i, 0), memory_space=pltpu.SMEM)

    def body(*refs):
        runs_kernel(owned, *refs)

    v, t, s, bins, regs = (in_hbm(x) for x in (v, t, s, bins, regs))
    return pl.pallas_call(
        body,
        grid=(steps,),
        in_specs=[far, far, far, flat, flat, flat_scalar],
        out_specs=[VMEM_WHOLE] * 5 + [SMEM_WHOLE],
        out_shape=[
            pltpu.VMEM((count + 1, LEVEL_ROWS, LANES), BF16),
            pltpu.VMEM((count + 1, 2, 16, LANES), BF16),
            pltpu.VMEM((3, chunks, LEVEL_ROWS, LANES), F32),
            pltpu.VMEM((chunks, 2, 16, LANES), BF16),
            pltpu.VMEM((16, 2 * LEVEL_ROWS, 2 * LANES), F32),
            jax.ShapeDtypeStruct((EDGE_AT + chunks,), jnp.int32),
        ],
        scratch_shapes=[
            pltpu.VMEM((steps, levels, ROWS, cols), BF16),
            pltpu.VMEM((steps, levels, ROWS, cols), BF16),
            pltpu.VMEM((steps, levels, ROWS, cols), F32),
            pltpu.VMEM((chunks, LEVEL_ROWS * PITCH, LANES), F32),
            pltpu.VMEM((chunks, LEVEL_ROWS * ROWS, LANES), F32),
            pltpu.SMEM((17,), jnp.int32),
            pltpu.SMEM((1,), jnp.int32),
            pltpu.SemaphoreType.DMA((3, steps)),
        ],
        compiler_params=pltpu.CompilerParams(vmem_limit_bytes=32 * 1024 * 1024),
        name="runs", cost_estimate=pl.CostEstimate(flops=4000000000, bytes_accessed=20000000, transcendentals=0),
    )(v, t, s, bins, regs, bins)


def local_sums(lists, place, halo, runs, tags, edge, edge_tags, begun):
    owners = begun.shape[0]
    values = [in_vmem(x) for x in (halo, runs, tags, edge, edge_tags, begun)]
    return pl.pallas_call(
        sums_kernel,
        in_specs=[SMEM_WHOLE, SMEM_WHOLE] + [VMEM_WHOLE] * 6,
        out_specs=[VMEM_WHOLE] * 3,
        out_shape=[
            pltpu.VMEM(begun.shape, F32),
            pltpu.VMEM((owners, LEVEL_ROWS, 2 * LANES), F32),
            pltpu.VMEM((owners, LEVEL_ROWS, 2 * LANES), BF16),
        ],
        input_output_aliases={7: 0},
        scratch_shapes=[pltpu.VMEM((LEVEL_ROWS, halo.shape[1]), F32)],
        compiler_params=pltpu.CompilerParams(vmem_limit_bytes=8 * 1024 * 1024),
        name="sums", cost_estimate=pl.CostEstimate(flops=4000000000, bytes_accessed=1000, transcendentals=0),
    )(lists, place, *values)[1:]


def assemble_kernel(scale, core_ref, mine_ref, other_ref, level_ref, total_ref):
    owners = mine_ref.shape[0]
    rows = level_ref.shape[1]
    owned = (BINS + owners - 1) // owners
    step = pl.program_id(0)
    first = core_ref[0] == 0
    lane = lax.broadcasted_iota(jnp.int32, (rows, LANES), 1)
    here = pl.ds(pl.multiple_of(step * rows, rows), rows)

    @pl.when(step == 0)
    def _():
        total_ref[...] = jnp.zeros_like(total_ref)

    def piece(o, q):
        side = slice((q % 2) * LANES, (q % 2 + 1) * LANES)
        a = mine_ref[o, here, side].astype(F32)
        b = other_ref[o, here, side].astype(F32)
        return jnp.where(first == (q < 2), a, b)

    tiles = (BINS + LANES - 1) // LANES
    for w in range(tiles):
        start = w * LANES
        width = min(LANES, BINS - start)
        regions = []
        for q in range(4):
            built = None
            for o in range(owners):
                lo = o * owned - start
                if lo >= width or lo + owned <= 0:
                    continue
                part = piece(o, q)
                if lo % LANES:
                    part = pltpu.roll(part, lo % LANES, 1)
                built = part if built is None else jnp.where(lane >= lo, part, built)
            regions.append(built)
        outs = [
            regions[0] + regions[1] + regions[2] + regions[3],
            regions[0],
            regions[1] + regions[2],
            regions[1],
            regions[2],
        ]
        for n in range(5):
            scaled = outs[n] * scale
            level_ref[n, :, start : start + width] = scaled[:, :width]
            total_ref[n : n + 1, start : start + width] += jnp.sum(
                scaled, axis=0, keepdims=True
            )[:, :width]


def assemble(core, mine, other, levels, scale):
    rows = LEVEL_ROWS // 2
    vmem = pl.BlockSpec(memory_space=pltpu.VMEM)

    def body(*refs):
        assemble_kernel(scale, *refs)

    return pl.pallas_call(
        body,
        grid=(LEVEL_ROWS // rows,),
        in_specs=[pl.BlockSpec(memory_space=pltpu.SMEM), vmem, vmem],
        out_specs=[
            pl.BlockSpec((5, rows, BINS), lambda i: (0, i, 0)),
            pl.BlockSpec((5, BINS), lambda i: (0, 0)),
        ],
        out_shape=[
            jax.ShapeDtypeStruct((5, levels, BINS), F32),
            jax.ShapeDtypeStruct((5, BINS), F32),
        ],
        name="assemble",
    )(core, in_vmem(mine), in_vmem(other))


def shards(v, t, s, bins, regs):
    levels, rows, cols = v.shape
    owners = lax.axis_size("gy")
    count = lax.axis_size("gx")
    owned = (BINS + owners - 1) // owners
    check_owner_rule(owned)
    scale = 0.5 * (BINS / (rows * owners * cols * count)) ** 0.5
    core = lax.rem(lax.axis_index("gx"), 2).reshape(1)

    def swapped(x, bit):
        return lax.ppermute(x, "gx", [(k, k ^ bit) for k in range(count)])

    is_last = (lax.axis_index("gy") == owners - 1).astype(jnp.int32)
    place = jnp.concatenate([core, is_last.reshape(1)])
    halo = lax.ppermute(t[:, 0, :], "gy", [(k, (k - 1) % owners) for k in range(owners)])
    runs, tags, edge, edge_tags, begun, lists = local_runs(v, t, s, bins, regs, owned)
    keep, send = local_sums(lists, place, halo, runs, tags, edge, edge_tags, begun)
    paired = (keep + swapped(send, 1).astype(F32)).astype(BF16)
    arrived = lax.all_to_all(paired, "gy", 0, 0, tiled=True)
    own = arrived.astype(F32).sum(axis=0).astype(BF16)
    near, far, back = (
        lax.ppermute(own, "gx", [(k, (k + 2 * d) % count) for k in range(count)]).astype(F32)
        for d in (1, 2, 3)
    )
    whole = ((own.astype(F32) + far) + (near + back)).astype(BF16)
    spread = jnp.broadcast_to(whole[None], (owners, *whole.shape))
    mine = lax.all_to_all(spread, "gy", 0, 0, tiled=True)
    other = swapped(mine, 1)
    return tuple(assemble(core, mine, other, levels, scale))


def solution(mesh):
    return jax.shard_map(
        shards,
        mesh=mesh,
        in_specs=(
            P(None, "gy", "gx"),
            P(None, "gy", "gx"),
            P(None, "gy", "gx"),
            P("gy", "gx"),
            P("gy", "gx"),
        ),
        out_specs=(P(), P()),
        check_vma=False,
    )
```

```python
import jax
import jax.numpy as jnp
from jax import lax
from jax.experimental import pallas as pl
from jax.experimental.pallas import tpu as pltpu
from jax.sharding import PartitionSpec as P

BINS = 1800
ROWS = 8
PITCH = 9
AHEAD = 3
LANES = 128
LEVEL_ROWS = 80
GROUP = 2
GROUPS = 134
UNROLL = 8
EACH_STEP = 16
OWNERS_AT = GROUP * (GROUPS + 1)
TRASH_AT = OWNERS_AT + GROUPS + 1
READY_AT = TRASH_AT + 2
HEAD_AT = READY_AT + GROUPS + 16
COUNT_AT = HEAD_AT + 1
EDGE_AT = COUNT_AT + 1
BF16 = jnp.bfloat16
F32 = jnp.float32


def owner_of(bins, owned):
    factor = (1 << 16) // owned + 1
    return lax.shift_right_logical(bins * factor, 16)


def check_owner_rule(owned):
    factor = (1 << 16) // owned + 1
    assert all((b * factor) >> 16 == b // owned for b in range(BINS))


def runs_kernel(
    owned, v_hbm, t_hbm, s_hbm, bin_ref, reg_ref, first_ref,
    runs_ref, tags_ref, edge_ref, edge_tags_ref, acc_ref, lists_ref,
    v_all, t_all, s_all, flux_ref, carry_ref, open_ref, used_ref, sem_ref,
):
    steps, levels = v_all.shape[:2]
    chunks = v_all.shape[3] // LANES
    spare = runs_ref.shape[0] - 1
    step = pl.program_id(0)
    last = steps - 1
    block = last - step
    v_ref, t_ref, s_ref = v_all.at[step], t_all.at[step], s_all.at[step]

    def copies(i):
        rows = pl.ds(pl.multiple_of((last - i) * ROWS, ROWS), ROWS)
        return [
            pltpu.make_async_copy(far.at[:, rows, :], near.at[i], sem_ref.at[n, i])
            for n, (far, near) in enumerate(((t_hbm, t_all), (v_hbm, v_all), (s_hbm, s_all)))
        ]

    @pl.when(step == 0)
    def _():
        for i in range(AHEAD):
            for copy in copies(i):
                copy.start()

        carry_ref[...] = jnp.zeros_like(carry_ref)
        acc_ref[...] = jnp.zeros_like(acc_ref)
        lists_ref[HEAD_AT] = 0
        lists_ref[COUNT_AT] = 0
        flux_ref[...] = jnp.zeros_like(flux_ref)
        runs_ref[spare] = jnp.zeros((LEVEL_ROWS, LANES), BF16)
        tags_ref[spare, 0] = jnp.full((16, LANES), -1, BF16)
        tags_ref[spare, 1] = jnp.zeros((16, LANES), BF16)
        used_ref[0] = 0

        for n in range(OWNERS_AT):
            lists_ref[n] = spare
        for n in range(OWNERS_AT, TRASH_AT):
            lists_ref[n] = 0
        for o in range(17):
            open_ref[o] = -1

    for copy in copies(step):
        copy.wait()

    @pl.when(step < steps - AHEAD)
    def _():
        for copy in copies(step + AHEAD):
            copy.start()

    @pl.when(step == 0)
    def _():
        for c in range(chunks):
            cols = slice(c * LANES, (c + 1) * LANES)
            for n, ref in enumerate((t_ref, v_ref, s_ref)):
                for k in range(levels):
                    flux_ref[c, k * PITCH : k * PITCH + ROWS, :] = ref[k, :, cols].astype(F32)
                edge_ref[n, c] = flux_ref[c, pl.ds(ROWS - 1, LEVEL_ROWS, stride=PITCH), :]

    def enlist(r, c):
        live = True if r < ROWS - 1 else step > 0
        own = owner_of(first_ref[r, c * LANES], owned)
        if r == ROWS - 1:
            lists_ref[jnp.where(live, TRASH_AT + 1, EDGE_AT + c)] = own
        key = own if r < ROWS - 1 else jnp.where(live, own, 16)
        held = open_ref[key]
        used = used_ref[0]
        is_open = held >= 0
        spot = jnp.where(is_open, held, GROUP * used)
        if r == ROWS - 1:
            lists_ref[jnp.where(live, spot, TRASH_AT)] = (block * ROWS + r) * chunks + c
            lists_ref[jnp.where(live, OWNERS_AT + lax.shift_right_logical(spot, 1), TRASH_AT)] = own
            full = ((spot + 1) & (GROUP - 1)) == 0
            open_ref[key] = jnp.where(live & ~full, spot + 1, -1)
            used_ref[0] = used + jnp.where(live & ~is_open, 1, 0)
            full = full & live
        else:
            lists_ref[spot] = (block * ROWS + r) * chunks + c
            lists_ref[OWNERS_AT + lax.shift_right_logical(spot, 1)] = own
            full = ((spot + 1) & (GROUP - 1)) == 0
            open_ref[key] = jnp.where(full, -1, spot + 1)
            used_ref[0] = used + jnp.where(is_open, 0, 1)
        ready = lists_ref[COUNT_AT]
        lists_ref[READY_AT + ready] = lax.shift_right_logical(spot, 1)
        lists_ref[COUNT_AT] = ready + jnp.where(full, 1, 0)

    def main_part(each):
        head = lists_ref[HEAD_AT]
        finished = lists_ref[COUNT_AT]
        lists_ref[HEAD_AT] = jnp.minimum(head + each, finished)
        chosen = [
            jnp.where(head + q < finished, lists_ref[READY_AT + head + q], GROUPS)
            for q in range(each)
        ]
        slot = slots()
        turn = 0

        waiting = [(r, c) for r in range(ROWS) for c in range(chunks)]
        is_last_row = lax.broadcasted_iota(jnp.int32, (1, ROWS, LANES), 1) == ROWS - 1
        for c in range(chunks):
            cols = slice(c * LANES, (c + 1) * LANES)
            for k in range(0, levels, 5):
                here = slice(k, k + 5)
                flat = slice(k * ROWS, (k + 5) * ROWS)
                warm = t_ref[here, :, cols].astype(F32)
                rolled = pltpu.roll(warm, ROWS - 1, 1)
                carried = carry_ref[c, flat, :].reshape(5, ROWS, LANES)
                below = jnp.where(is_last_row, carried, rolled)
                carry_ref[c, flat, :] = rolled.reshape(5 * ROWS, LANES)
                flux = v_ref[here, :, cols].astype(F32) * (warm + below) * s_ref[here, :, cols]
                for q in range(5):
                    at = (k + q) * PITCH
                    flux_ref[c, at : at + ROWS, :] = flux[q]
                if waiting:
                    enlist(*waiting.pop(0))
                if turn % 3 == 1 and chosen:
                    add_group(lists_ref, chosen.pop(0), slot, runs_ref, tags_ref, acc_ref)
                turn += 1
            for r in range(ROWS):
                cells = flux_ref[c, pl.ds(r, LEVEL_ROWS, stride=PITCH), :]
                runs_ref[(block * ROWS + r) * chunks + c] = cells.astype(BF16)

    @pl.when(step == 0)
    def _():
        main_part(0)

    @pl.when(step > 0)
    def _():
        main_part(EACH_STEP)

    bins = bin_ref[...]
    regs = reg_ref[...]
    code = bins - owner_of(bins, owned) * owned + (regs & 1) * LANES
    code = code.astype(F32)
    high = lax.shift_right_logical(regs, 1).astype(F32)
    for r in range(ROWS):
        for c in range(chunks):
            cols = slice(c * LANES, (c + 1) * LANES)
            run = (block * ROWS + r) * chunks + c
            tags_ref[run, 0] = jnp.broadcast_to(code[r : r + 1, cols], (16, LANES)).astype(BF16)
            tags_ref[run, 1] = jnp.broadcast_to(high[r : r + 1, cols], (16, LANES)).astype(BF16)

    @pl.when(step == 0)
    def _():
        edge_tags_ref[...] = tags_ref[spare - chunks : spare]

    @pl.when(step == last)
    def _():
        for o in range(16):
            held = open_ref[o]
            ready = lists_ref[COUNT_AT]
            lists_ref[READY_AT + ready] = lax.shift_right_logical(held, 1)
            lists_ref[COUNT_AT] = ready + jnp.where(held >= 0, 1, 0)
        ready = lists_ref[COUNT_AT]
        for n in range(UNROLL):
            lists_ref[READY_AT + ready + n] = GROUPS


def stacked(x, n):
    return jnp.concatenate([x] * n, axis=0)


def group_sums(slot, tags_ref, members):
    lows, highs, spots = [], [], []
    one = jnp.ones((2 * LANES, LANES), BF16)
    nothing = jnp.zeros((2 * LANES, LANES), BF16)
    for cells, run in members:
        upper = cells * stacked(tags_ref[run, 1], LEVEL_ROWS // 16)
        lows.append(cells - upper)
        highs.append(upper)
        spots.append(jnp.where(slot == stacked(tags_ref[run, 0], 2 * LANES // 16), one, nothing))
    left = jnp.concatenate([jnp.concatenate(lows, axis=1), jnp.concatenate(highs, axis=1)], axis=0)
    right = jnp.concatenate(spots, axis=1)
    return lax.dot_general(left, right, (((1,), (1,)), ((), ())), preferred_element_type=F32)


def slots():
    return lax.broadcasted_iota(jnp.int32, (2 * LANES, LANES), 0).astype(F32).astype(BF16)


def add_group(lists_ref, group, slot, runs_ref, tags_ref, acc_ref):
    names = [lists_ref[GROUP * group + k] for k in range(GROUP)]
    own = lists_ref[OWNERS_AT + group]
    acc_ref[own] += group_sums(slot, tags_ref, [(runs_ref[a], a) for a in names])


def sums_kernel(
    lists_ref, place_ref, halo_ref, runs_ref, tags_ref, edge_ref, edge_tags_ref, begun_ref,
    acc_ref, keep_ref, send_ref, halo32_ref,
):
    del begun_ref
    levels, cols = halo_ref.shape
    owners = acc_ref.shape[0]
    slot = slots()
    head = lists_ref[HEAD_AT]
    count = lists_ref[COUNT_AT]
    halo = jnp.where(place_ref[1] == 0, halo_ref[...].astype(F32), 0.0)
    halo32_ref[:levels] = halo
    halo32_ref[levels:] = jnp.zeros((LEVEL_ROWS - levels, cols), F32)

    def several(n, _):
        for u in range(UNROLL):
            group = lists_ref[READY_AT + head + n * UNROLL + u]
            add_group(lists_ref, group, slot, runs_ref, tags_ref, acc_ref)
        return 0

    lax.fori_loop(0, lax.div(count - head + UNROLL - 1, UNROLL), several, 0)

    for c in range(cols // LANES):
        warm = edge_ref[0, c] + halo32_ref[:, c * LANES : (c + 1) * LANES]
        flux = (edge_ref[1, c] * warm * edge_ref[2, c]).astype(BF16)
        acc_ref[lists_ref[EDGE_AT + c]] += group_sums(slot, edge_tags_ref, [(flux, c)])
    core = place_ref[0]
    mine = pl.multiple_of(core * LEVEL_ROWS, LEVEL_ROWS)
    others = pl.multiple_of((1 - core) * LEVEL_ROWS, LEVEL_ROWS)
    for o in range(owners):
        keep_ref[o] = acc_ref[o, pl.ds(mine, LEVEL_ROWS), :]
        send_ref[o] = acc_ref[o, pl.ds(others, LEVEL_ROWS), :].astype(BF16)


def in_vmem(x):
    return pltpu.with_memory_space_constraint(x, pltpu.VMEM)


def in_hbm(x):
    return pltpu.with_memory_space_constraint(x, pltpu.HBM)


SMEM_WHOLE = pl.BlockSpec(memory_space=pltpu.SMEM)
VMEM_WHOLE = pl.BlockSpec(memory_space=pltpu.VMEM)


def local_runs(v, t, s, bins, regs, owned):
    levels, rows, cols = v.shape
    steps = rows // ROWS
    chunks = cols // LANES
    count = rows * chunks
    far = pl.BlockSpec(memory_space=pltpu.HBM)
    flat = pl.BlockSpec((ROWS, cols), lambda i: (steps - 1 - i, 0))
    flat_scalar = pl.BlockSpec((ROWS, cols), lambda i: (steps - 1 - i, 0), memory_space=pltpu.SMEM)

    def body(*refs):
        runs_kernel(owned, *refs)

    v, t, s, bins, regs = (in_hbm(x) for x in (v, t, s, bins, regs))
    return pl.pallas_call(
        body,
        grid=(steps,),
        in_specs=[far, far, far, flat, flat, flat_scalar],
        out_specs=[VMEM_WHOLE] * 5 + [SMEM_WHOLE],
        out_shape=[
            pltpu.VMEM((count + 1, LEVEL_ROWS, LANES), BF16),
            pltpu.VMEM((count + 1, 2, 16, LANES), BF16),
            pltpu.VMEM((3, chunks, LEVEL_ROWS, LANES), F32),
            pltpu.VMEM((chunks, 2, 16, LANES), BF16),
            pltpu.VMEM((16, 2 * LEVEL_ROWS, 2 * LANES), F32),
            jax.ShapeDtypeStruct((EDGE_AT + chunks,), jnp.int32),
        ],
        scratch_shapes=[
            pltpu.VMEM((steps, levels, ROWS, cols), BF16),
            pltpu.VMEM((steps, levels, ROWS, cols), BF16),
            pltpu.VMEM((steps, levels, ROWS, cols), F32),
            pltpu.VMEM((chunks, LEVEL_ROWS * PITCH, LANES), F32),
            pltpu.VMEM((chunks, LEVEL_ROWS * ROWS, LANES), F32),
            pltpu.SMEM((17,), jnp.int32),
            pltpu.SMEM((1,), jnp.int32),
            pltpu.SemaphoreType.DMA((3, steps)),
        ],
        compiler_params=pltpu.CompilerParams(vmem_limit_bytes=32 * 1024 * 1024),
        name="runs", cost_estimate=pl.CostEstimate(flops=4000000000, bytes_accessed=20000000, transcendentals=0),
    )(v, t, s, bins, regs, bins)


def local_sums(lists, place, halo, runs, tags, edge, edge_tags, begun):
    owners = begun.shape[0]
    values = [in_vmem(x) for x in (halo, runs, tags, edge, edge_tags, begun)]
    return pl.pallas_call(
        sums_kernel,
        in_specs=[SMEM_WHOLE, SMEM_WHOLE] + [VMEM_WHOLE] * 6,
        out_specs=[VMEM_WHOLE] * 3,
        out_shape=[
            pltpu.VMEM(begun.shape, F32),
            pltpu.VMEM((owners, LEVEL_ROWS, 2 * LANES), F32),
            pltpu.VMEM((owners, LEVEL_ROWS, 2 * LANES), BF16),
        ],
        input_output_aliases={7: 0},
        scratch_shapes=[pltpu.VMEM((LEVEL_ROWS, halo.shape[1]), F32)],
        compiler_params=pltpu.CompilerParams(vmem_limit_bytes=8 * 1024 * 1024),
        name="sums", cost_estimate=pl.CostEstimate(flops=4000000000, bytes_accessed=1000, transcendentals=0),
    )(lists, place, *values)[1:]


def assemble_kernel(scale, core_ref, mine_ref, other_ref, level_ref, total_ref):
    owners = mine_ref.shape[0]
    rows = level_ref.shape[1]
    owned = (BINS + owners - 1) // owners
    step = pl.program_id(0)
    first = core_ref[0] == 0
    lane = lax.broadcasted_iota(jnp.int32, (rows, LANES), 1)
    here = pl.ds(pl.multiple_of(step * rows, rows), rows)

    @pl.when(step == 0)
    def _():
        total_ref[...] = jnp.zeros_like(total_ref)

    def piece(o, q):
        side = slice((q % 2) * LANES, (q % 2 + 1) * LANES)
        a = mine_ref[o, here, side].astype(F32)
        b = other_ref[o, here, side].astype(F32)
        return jnp.where(first == (q < 2), a, b)

    tiles = (BINS + LANES - 1) // LANES
    for w in range(tiles):
        start = w * LANES
        width = min(LANES, BINS - start)
        regions = []
        for q in range(4):
            built = None
            for o in range(owners):
                lo = o * owned - start
                if lo >= width or lo + owned <= 0:
                    continue
                part = piece(o, q)
                if lo % LANES:
                    part = pltpu.roll(part, lo % LANES, 1)
                built = part if built is None else jnp.where(lane >= lo, part, built)
            regions.append(built)
        outs = [
            regions[0] + regions[1] + regions[2] + regions[3],
            regions[0],
            regions[1] + regions[2],
            regions[1],
            regions[2],
        ]
        for n in range(5):
            scaled = outs[n] * scale
            level_ref[n, :, start : start + width] = scaled[:, :width]
            total_ref[n : n + 1, start : start + width] += jnp.sum(
                scaled, axis=0, keepdims=True
            )[:, :width]


def assemble(core, mine, other, levels, scale):
    rows = LEVEL_ROWS // 2
    vmem = pl.BlockSpec(memory_space=pltpu.VMEM)

    def body(*refs):
        assemble_kernel(scale, *refs)

    return pl.pallas_call(
        body,
        grid=(LEVEL_ROWS // rows,),
        in_specs=[pl.BlockSpec(memory_space=pltpu.SMEM), vmem, vmem],
        out_specs=[
            pl.BlockSpec((5, rows, BINS), lambda i: (0, i, 0)),
            pl.BlockSpec((5, BINS), lambda i: (0, 0)),
        ],
        out_shape=[
            jax.ShapeDtypeStruct((5, levels, BINS), F32),
            jax.ShapeDtypeStruct((5, BINS), F32),
        ],
        name="assemble",
    )(core, in_vmem(mine), in_vmem(other))


def shards(v, t, s, bins, regs):
    levels, rows, cols = v.shape
    owners = lax.axis_size("gy")
    count = lax.axis_size("gx")
    owned = (BINS + owners - 1) // owners
    check_owner_rule(owned)
    scale = 0.5 * (BINS / (rows * owners * cols * count)) ** 0.5
    core = lax.rem(lax.axis_index("gx"), 2).reshape(1)

    def swapped(x, bit):
        return lax.ppermute(x, "gx", [(k, k ^ bit) for k in range(count)])

    is_last = (lax.axis_index("gy") == owners - 1).astype(jnp.int32)
    place = jnp.concatenate([core, is_last.reshape(1)])
    halo = lax.ppermute(t[:, 0, :], "gy", [(k, (k - 1) % owners) for k in range(owners)])
    runs, tags, edge, edge_tags, begun, lists = local_runs(v, t, s, bins, regs, owned)
    keep, send = local_sums(lists, place, halo, runs, tags, edge, edge_tags, begun)
    paired = (keep + swapped(send, 1).astype(F32)).astype(BF16)
    arrived = lax.all_to_all(paired, "gy", 0, 0, tiled=True)
    own = arrived.astype(F32).sum(axis=0).astype(BF16)
    near, far, back = (
        lax.ppermute(own, "gx", [(k, (k + 2 * d) % count) for k in range(count)]).astype(F32)
        for d in (1, 2, 3)
    )
    whole = ((own.astype(F32) + far) + (near + back)).astype(BF16)
    spread = jnp.broadcast_to(whole[None], (owners, *whole.shape))
    mine = lax.all_to_all(spread, "gy", 0, 0, tiled=True)
    other = swapped(mine, 1)
    return tuple(assemble(core, mine, other, levels, scale))


def solution(mesh):
    return jax.shard_map(
        shards,
        mesh=mesh,
        in_specs=(
            P(None, "gy", "gx"),
            P(None, "gy", "gx"),
            P(None, "gy", "gx"),
            P("gy", "gx"),
            P("gy", "gx"),
        ),
        out_specs=(P(), P()),
        check_vma=False,
    )
```

```python
import jax
import jax.numpy as jnp
from jax import lax
from jax.experimental import pallas as pl
from jax.experimental.pallas import tpu as pltpu
from jax.sharding import PartitionSpec as P


BINS = 1800
ROWS = 8
PITCH = 9
AHEAD = 3
LANES = 128
LEVEL_ROWS = 80
GROUP = 4
GROUPS = 75
UNROLL = 5
EACH_STEP = 8
OWNERS_AT = GROUP * (GROUPS + 1)
TRASH_AT = OWNERS_AT + GROUPS + 1
READY_AT = TRASH_AT + 2
HEAD_AT = READY_AT + GROUPS + 16
COUNT_AT = HEAD_AT + 1
EDGE_AT = COUNT_AT + 1
BF16 = jnp.bfloat16
F32 = jnp.float32


def owner_of(bins, owned):
    factor = (1 << 16) // owned + 1
    return lax.shift_right_logical(bins * factor, 16)


def check_owner_rule(owned):
    factor = (1 << 16) // owned + 1
    assert all((b * factor) >> 16 == b // owned for b in range(BINS))


def runs_kernel(
    owned, v_hbm, t_hbm, s_hbm, bin_ref, reg_ref, first_ref,
    runs_ref, tags_ref, edge_ref, edge_tags_ref, acc_ref, lists_ref,
    v_all, t_all, s_all, flux_ref, carry_ref, open_ref, used_ref, sem_ref,
):
    steps, levels = v_all.shape[:2]
    chunks = v_all.shape[3] // LANES
    spare = runs_ref.shape[0] - 1
    step = pl.program_id(0)
    last = steps - 1
    block = last - step
    v_ref, t_ref, s_ref = v_all.at[step], t_all.at[step], s_all.at[step]

    def copies(i):
        rows = pl.ds(pl.multiple_of((last - i) * ROWS, ROWS), ROWS)
        return [
            pltpu.make_async_copy(far.at[:, rows, :], near.at[i], sem_ref.at[n, i])
            for n, (far, near) in enumerate(((t_hbm, t_all), (v_hbm, v_all), (s_hbm, s_all)))
        ]

    @pl.when(step == 0)
    def _():
        for i in range(AHEAD):
            for copy in copies(i):
                copy.start()

        carry_ref[...] = jnp.zeros_like(carry_ref)
        acc_ref[...] = jnp.zeros_like(acc_ref)
        lists_ref[HEAD_AT] = 0
        lists_ref[COUNT_AT] = 0
        flux_ref[...] = jnp.zeros_like(flux_ref)
        runs_ref[spare] = jnp.zeros((LEVEL_ROWS, LANES), BF16)
        tags_ref[spare, 0] = jnp.full((16, LANES), -1, BF16)
        tags_ref[spare, 1] = jnp.zeros((16, LANES), BF16)
        used_ref[0] = 0

        for n in range(OWNERS_AT):
            lists_ref[n] = spare
        for n in range(OWNERS_AT, TRASH_AT):
            lists_ref[n] = 0
        for o in range(17):
            open_ref[o] = -1

    for copy in copies(step):
        copy.wait()

    @pl.when(step < steps - AHEAD)
    def _():
        for copy in copies(step + AHEAD):
            copy.start()

    @pl.when(step == 0)
    def _():
        for c in range(chunks):
            cols = slice(c * LANES, (c + 1) * LANES)
            for n, ref in enumerate((t_ref, v_ref, s_ref)):
                for k in range(levels):
                    flux_ref[c, k * PITCH : k * PITCH + ROWS, :] = ref[k, :, cols].astype(F32)
                edge_ref[n, c] = flux_ref[c, pl.ds(ROWS - 1, LEVEL_ROWS, stride=PITCH), :]

    def enlist(r, c):
        live = True if r < ROWS - 1 else step > 0
        own = owner_of(first_ref[r, c * LANES], owned)
        if r == ROWS - 1:
            lists_ref[jnp.where(live, TRASH_AT + 1, EDGE_AT + c)] = own
        key = own if r < ROWS - 1 else jnp.where(live, own, 16)
        held = open_ref[key]
        used = used_ref[0]
        is_open = held >= 0
        spot = jnp.where(is_open, held, GROUP * used)
        if r == ROWS - 1:
            lists_ref[jnp.where(live, spot, TRASH_AT)] = (block * ROWS + r) * chunks + c
            lists_ref[jnp.where(live, OWNERS_AT + lax.shift_right_logical(spot, 2), TRASH_AT)] = own
            full = ((spot + 1) & (GROUP - 1)) == 0
            open_ref[key] = jnp.where(live & ~full, spot + 1, -1)
            used_ref[0] = used + jnp.where(live & ~is_open, 1, 0)
            full = full & live
        else:
            lists_ref[spot] = (block * ROWS + r) * chunks + c
            lists_ref[OWNERS_AT + lax.shift_right_logical(spot, 2)] = own
            full = ((spot + 1) & (GROUP - 1)) == 0
            open_ref[key] = jnp.where(full, -1, spot + 1)
            used_ref[0] = used + jnp.where(is_open, 0, 1)
        ready = lists_ref[COUNT_AT]
        lists_ref[READY_AT + ready] = lax.shift_right_logical(spot, 2)
        lists_ref[COUNT_AT] = ready + jnp.where(full, 1, 0)

    def main_part(each):
        head = lists_ref[HEAD_AT]
        finished = lists_ref[COUNT_AT]
        lists_ref[HEAD_AT] = jnp.minimum(head + each, finished)
        chosen = [
            jnp.where(head + q < finished, lists_ref[READY_AT + head + q], GROUPS)
            for q in range(each)
        ]
        slot = slots()
        turn = 0

        waiting = [(r, c) for r in range(ROWS) for c in range(chunks)]
        is_last_row = lax.broadcasted_iota(jnp.int32, (1, ROWS, LANES), 1) == ROWS - 1
        for c in range(chunks):
            cols = slice(c * LANES, (c + 1) * LANES)
            for k in range(0, levels, 5):
                here = slice(k, k + 5)
                flat = slice(k * ROWS, (k + 5) * ROWS)
                warm = t_ref[here, :, cols].astype(F32)
                rolled = pltpu.roll(warm, ROWS - 1, 1)
                carried = carry_ref[c, flat, :].reshape(5, ROWS, LANES)
                below = jnp.where(is_last_row, carried, rolled)
                carry_ref[c, flat, :] = rolled.reshape(5 * ROWS, LANES)
                flux = v_ref[here, :, cols].astype(F32) * (warm + below) * s_ref[here, :, cols]
                for q in range(5):
                    at = (k + q) * PITCH
                    flux_ref[c, at : at + ROWS, :] = flux[q]
                if waiting:
                    enlist(*waiting.pop(0))
                if turn % 5 == 2 and chosen:
                    add_group(lists_ref, chosen.pop(0), slot, runs_ref, tags_ref, acc_ref)
                turn += 1
            for r in range(ROWS):
                cells = flux_ref[c, pl.ds(r, LEVEL_ROWS, stride=PITCH), :]
                runs_ref[(block * ROWS + r) * chunks + c] = cells.astype(BF16)

    @pl.when(step == 0)
    def _():
        main_part(0)

    @pl.when(step > 0)
    def _():
        main_part(EACH_STEP)

    bins = bin_ref[...]
    regs = reg_ref[...]
    code = bins - owner_of(bins, owned) * owned + (regs & 1) * LANES
    code = code.astype(F32)
    high = lax.shift_right_logical(regs, 1).astype(F32)
    for r in range(ROWS):
        for c in range(chunks):
            cols = slice(c * LANES, (c + 1) * LANES)
            run = (block * ROWS + r) * chunks + c
            tags_ref[run, 0] = jnp.broadcast_to(code[r : r + 1, cols], (16, LANES)).astype(BF16)
            tags_ref[run, 1] = jnp.broadcast_to(high[r : r + 1, cols], (16, LANES)).astype(BF16)

    @pl.when(step == 0)
    def _():
        edge_tags_ref[...] = tags_ref[spare - chunks : spare]

    @pl.when(step == last)
    def _():
        for o in range(16):
            held = open_ref[o]
            ready = lists_ref[COUNT_AT]
            lists_ref[READY_AT + ready] = lax.shift_right_logical(held, 2)
            lists_ref[COUNT_AT] = ready + jnp.where(held >= 0, 1, 0)
        ready = lists_ref[COUNT_AT]
        for n in range(UNROLL):
            lists_ref[READY_AT + ready + n] = GROUPS


def stacked(x, n):
    return jnp.concatenate([x] * n, axis=0)


def group_sums(slot, tags_ref, members):
    lows, highs, spots = [], [], []
    one = jnp.ones((2 * LANES, LANES), BF16)
    nothing = jnp.zeros((2 * LANES, LANES), BF16)
    for cells, run in members:
        upper = cells * stacked(tags_ref[run, 1], LEVEL_ROWS // 16)
        lows.append(cells - upper)
        highs.append(upper)
        spots.append(jnp.where(slot == stacked(tags_ref[run, 0], 2 * LANES // 16), one, nothing))
    left = jnp.concatenate([jnp.concatenate(lows, axis=1), jnp.concatenate(highs, axis=1)], axis=0)
    right = jnp.concatenate(spots, axis=1)
    return lax.dot_general(left, right, (((1,), (1,)), ((), ())), preferred_element_type=F32)


def slots():
    return lax.broadcasted_iota(jnp.int32, (2 * LANES, LANES), 0).astype(F32).astype(BF16)


def add_group(lists_ref, group, slot, runs_ref, tags_ref, acc_ref):
    names = [lists_ref[GROUP * group + k] for k in range(GROUP)]
    own = lists_ref[OWNERS_AT + group]
    acc_ref[own] += group_sums(slot, tags_ref, [(runs_ref[a], a) for a in names])


def sums_kernel(
    lists_ref, place_ref, halo_ref, runs_ref, tags_ref, edge_ref, edge_tags_ref, begun_ref,
    acc_ref, keep_ref, send_ref, halo32_ref,
):
    del begun_ref
    levels, cols = halo_ref.shape
    owners = acc_ref.shape[0]
    slot = slots()
    head = lists_ref[HEAD_AT]
    count = lists_ref[COUNT_AT]
    halo = jnp.where(place_ref[1] == 0, halo_ref[...].astype(F32), 0.0)
    halo32_ref[:levels] = halo
    halo32_ref[levels:] = jnp.zeros((LEVEL_ROWS - levels, cols), F32)

    def several(n, _):
        for u in range(UNROLL):
            group = lists_ref[READY_AT + head + n * UNROLL + u]
            add_group(lists_ref, group, slot, runs_ref, tags_ref, acc_ref)
        return 0

    lax.fori_loop(0, lax.div(count - head + UNROLL - 1, UNROLL), several, 0)

    for c in range(cols // LANES):
        warm = edge_ref[0, c] + halo32_ref[:, c * LANES : (c + 1) * LANES]
        flux = (edge_ref[1, c] * warm * edge_ref[2, c]).astype(BF16)
        acc_ref[lists_ref[EDGE_AT + c]] += group_sums(slot, edge_tags_ref, [(flux, c)])
    core = place_ref[0]
    mine = pl.multiple_of(core * LEVEL_ROWS, LEVEL_ROWS)
    others = pl.multiple_of((1 - core) * LEVEL_ROWS, LEVEL_ROWS)
    for o in range(owners):
        keep_ref[o] = acc_ref[o, pl.ds(mine, LEVEL_ROWS), :]
        send_ref[o] = acc_ref[o, pl.ds(others, LEVEL_ROWS), :].astype(BF16)


def in_vmem(x):
    return pltpu.with_memory_space_constraint(x, pltpu.VMEM)


def in_hbm(x):
    return pltpu.with_memory_space_constraint(x, pltpu.HBM)


SMEM_WHOLE = pl.BlockSpec(memory_space=pltpu.SMEM)
VMEM_WHOLE = pl.BlockSpec(memory_space=pltpu.VMEM)


def local_runs(v, t, s, bins, regs, owned):
    levels, rows, cols = v.shape
    steps = rows // ROWS
    chunks = cols // LANES
    count = rows * chunks
    far = pl.BlockSpec(memory_space=pltpu.HBM)
    flat = pl.BlockSpec((ROWS, cols), lambda i: (steps - 1 - i, 0))
    flat_scalar = pl.BlockSpec((ROWS, cols), lambda i: (steps - 1 - i, 0), memory_space=pltpu.SMEM)

    def body(*refs):
        runs_kernel(owned, *refs)

    v, t, s, bins, regs = (in_hbm(x) for x in (v, t, s, bins, regs))
    return pl.pallas_call(
        body,
        grid=(steps,),
        in_specs=[far, far, far, flat, flat, flat_scalar],
        out_specs=[VMEM_WHOLE] * 5 + [SMEM_WHOLE],
        out_shape=[
            pltpu.VMEM((count + 1, LEVEL_ROWS, LANES), BF16),
            pltpu.VMEM((count + 1, 2, 16, LANES), BF16),
            pltpu.VMEM((3, chunks, LEVEL_ROWS, LANES), F32),
            pltpu.VMEM((chunks, 2, 16, LANES), BF16),
            pltpu.VMEM((16, 2 * LEVEL_ROWS, 2 * LANES), F32),
            jax.ShapeDtypeStruct((EDGE_AT + chunks,), jnp.int32),
        ],
        scratch_shapes=[
            pltpu.VMEM((steps, levels, ROWS, cols), BF16),
            pltpu.VMEM((steps, levels, ROWS, cols), BF16),
            pltpu.VMEM((steps, levels, ROWS, cols), F32),
            pltpu.VMEM((chunks, LEVEL_ROWS * PITCH, LANES), F32),
            pltpu.VMEM((chunks, LEVEL_ROWS * ROWS, LANES), F32),
            pltpu.SMEM((17,), jnp.int32),
            pltpu.SMEM((1,), jnp.int32),
            pltpu.SemaphoreType.DMA((3, steps)),
        ],
        compiler_params=pltpu.CompilerParams(vmem_limit_bytes=32 * 1024 * 1024),
        name="runs", cost_estimate=pl.CostEstimate(flops=4000000000, bytes_accessed=20000000, transcendentals=0),
    )(v, t, s, bins, regs, bins)


def local_sums(lists, place, halo, runs, tags, edge, edge_tags, begun):
    owners = begun.shape[0]
    values = [in_vmem(x) for x in (halo, runs, tags, edge, edge_tags, begun)]
    return pl.pallas_call(
        sums_kernel,
        in_specs=[SMEM_WHOLE, SMEM_WHOLE] + [VMEM_WHOLE] * 6,
        out_specs=[VMEM_WHOLE] * 3,
        out_shape=[
            pltpu.VMEM(begun.shape, F32),
            pltpu.VMEM((owners, LEVEL_ROWS, 2 * LANES), F32),
            pltpu.VMEM((owners, LEVEL_ROWS, 2 * LANES), BF16),
        ],
        input_output_aliases={7: 0},
        scratch_shapes=[pltpu.VMEM((LEVEL_ROWS, halo.shape[1]), F32)],
        compiler_params=pltpu.CompilerParams(vmem_limit_bytes=8 * 1024 * 1024),
        name="sums", cost_estimate=pl.CostEstimate(flops=4000000000, bytes_accessed=1000, transcendentals=0),
    )(lists, place, *values)[1:]


def assemble_kernel(scale, core_ref, mine_ref, other_ref, level_ref, total_ref):
    owners = mine_ref.shape[0]
    rows = level_ref.shape[1]
    owned = (BINS + owners - 1) // owners
    step = pl.program_id(0)
    first = core_ref[0] == 0
    lane = lax.broadcasted_iota(jnp.int32, (rows, LANES), 1)
    here = pl.ds(pl.multiple_of(step * rows, rows), rows)

    @pl.when(step == 0)
    def _():
        total_ref[...] = jnp.zeros_like(total_ref)

    def piece(o, q):
        side = slice((q % 2) * LANES, (q % 2 + 1) * LANES)
        a = mine_ref[o, here, side].astype(F32)
        b = other_ref[o, here, side].astype(F32)
        return jnp.where(first == (q < 2), a, b)

    tiles = (BINS + LANES - 1) // LANES
    for w in range(tiles):
        start = w * LANES
        width = min(LANES, BINS - start)
        regions = []
        for q in range(4):
            built = None
            for o in range(owners):
                lo = o * owned - start
                if lo >= width or lo + owned <= 0:
                    continue
                part = piece(o, q)
                if lo % LANES:
                    part = pltpu.roll(part, lo % LANES, 1)
                built = part if built is None else jnp.where(lane >= lo, part, built)
            regions.append(built)
        outs = [
            regions[0] + regions[1] + regions[2] + regions[3],
            regions[0],
            regions[1] + regions[2],
            regions[1],
            regions[2],
        ]
        for n in range(5):
            scaled = outs[n] * scale
            level_ref[n, :, start : start + width] = scaled[:, :width]
            total_ref[n : n + 1, start : start + width] += jnp.sum(
                scaled, axis=0, keepdims=True
            )[:, :width]


def assemble(core, mine, other, levels, scale):
    rows = LEVEL_ROWS // 2
    vmem = pl.BlockSpec(memory_space=pltpu.VMEM)

    def body(*refs):
        assemble_kernel(scale, *refs)

    return pl.pallas_call(
        body,
        grid=(LEVEL_ROWS // rows,),
        in_specs=[pl.BlockSpec(memory_space=pltpu.SMEM), vmem, vmem],
        out_specs=[
            pl.BlockSpec((5, rows, BINS), lambda i: (0, i, 0)),
            pl.BlockSpec((5, BINS), lambda i: (0, 0)),
        ],
        out_shape=[
            jax.ShapeDtypeStruct((5, levels, BINS), F32),
            jax.ShapeDtypeStruct((5, BINS), F32),
        ],
        name="assemble",
    )(core, in_vmem(mine), in_vmem(other))


def shards(v, t, s, bins, regs):
    levels, rows, cols = v.shape
    owners = lax.axis_size("gy")
    count = lax.axis_size("gx")
    owned = (BINS + owners - 1) // owners
    check_owner_rule(owned)
    scale = 0.5 * (BINS / (rows * owners * cols * count)) ** 0.5
    core = lax.rem(lax.axis_index("gx"), 2).reshape(1)

    def swapped(x, bit):
        return lax.ppermute(x, "gx", [(k, k ^ bit) for k in range(count)])

    is_last = (lax.axis_index("gy") == owners - 1).astype(jnp.int32)
    place = jnp.concatenate([core, is_last.reshape(1)])
    halo = lax.ppermute(t[:, 0, :], "gy", [(k, (k - 1) % owners) for k in range(owners)])
    runs, tags, edge, edge_tags, begun, lists = local_runs(v, t, s, bins, regs, owned)
    keep, send = local_sums(lists, place, halo, runs, tags, edge, edge_tags, begun)
    paired = (keep + swapped(send, 1).astype(F32)).astype(BF16)
    arrived = lax.all_to_all(paired, "gy", 0, 0, tiled=True)
    own = arrived.astype(F32).sum(axis=0).astype(BF16)

    def turned(d):
        moved = lax.ppermute(own, "gx", [(k, (k + 2 * d) % count) for k in range(count)])
        return moved.astype(F32)

    far, near, back = turned(2), turned(1), turned(3)
    whole = ((own.astype(F32) + far) + (near + back)).astype(BF16)
    spread = jnp.broadcast_to(whole[None], (owners, *whole.shape))
    mine = lax.all_to_all(spread, "gy", 0, 0, tiled=True)
    other = swapped(mine, 1)
    return tuple(assemble(core, mine, other, levels, scale))


def solution(mesh):
    return jax.shard_map(
        shards,
        mesh=mesh,
        in_specs=(
            P(None, "gy", "gx"),
            P(None, "gy", "gx"),
            P(None, "gy", "gx"),
            P("gy", "gx"),
            P("gy", "gx"),
        ),
        out_specs=(P(), P()),
        check_vma=False,
    )
```
